256 devices in a mesh: grp: 8 (over z_lo, x), ty: 8 (over z_hi, core), tx: 4 (over y).
Axes of the slice: x: 4, y: 4, z: 8 (z_hi: 4, z_lo: 2; z = z_hi * 2 + z_lo), core: 2. Of those that a mesh axis runs over, the one named last changes fastest.
Arguments:
- noisy: float32 [4, 2048, 1024], P(None, ('grp', 'ty'), 'tx'), may hold values from -6 to 6
- w_in: float32 [64, 4], replicated, may hold values from -3 to 3
- k_first: bfloat16 [3, 3, 64, 64], replicated, may hold values from -0.25 to 0.25
- w_down: bfloat16 [256, 64], replicated, may hold values from -0.75 to 0.75
- k_coarse: bfloat16 [3, 3, 256, 256], replicated, may hold values from -0.125 to 0.125
- w_up: bfloat16 [64, 256], replicated, may hold values from -0.375 to 0.375
- k_last: bfloat16 [3, 3, 64, 64], replicated, may hold values from -0.25 to 0.25
- w_out: bfloat16 [4, 64], replicated, may hold values from -0.75 to 0.75
- station_cell: int32 [64, 4, 128], P(('grp', 'ty'), 'tx'), may hold values from 0 to 8191
- station_count: int32 [64, 4, 128], P(('grp', 'ty'), 'tx'), may hold values from 0 to 3
- observed: float32 [4, 64, 4, 128], P(None, ('grp', 'ty'), 'tx'), may hold values from -6 to 6
Outputs:
- next_state: float32 [4, 2048, 1024], P(None, ('grp', 'ty'), 'tx')
The draws below stay inside these ranges and needn't reach their ends.
Inputs may be any that keep to these rules, and one draw needn't show every extreme that they name: `station_count`: a count of 0 marks a station without a valid report; several stations may share a cell.
All inputs are finite; a program needn't handle non-finite values.
Results may differ from the reference program's by a relative error of at most 0.017.
Values may be sent and summed in bfloat16 or wider, within the bound.
A program may use at most 64 MiB of HBM per device.

```python
import jax
import jax.numpy as jnp
from jax import lax

V = 4
C0 = 64
C1 = 256
POOL = 32
H_DEV = 32
W_DEV = 256
STA = 128
BROWS = 64
BCOLS = 4
NY = 2048
NX = 1024


def draw_noisy(key, part):
    base = jax.random.fold_in(key, 7101)
    rough_key, offset_key = jax.random.split(base)
    coarse_shape = (V, NY // POOL, NX // POOL)
    rough = jax.random.normal(rough_key, (V, NY, NX), jnp.float32)
    offset = jax.random.uniform(offset_key, coarse_shape, jnp.float32, -3.0, 3.0)
    spread = jnp.repeat(jnp.repeat(offset, POOL, axis=1), POOL, axis=2)
    return jnp.clip(rough + spread, -6.0, 6.0)


def set_ends(entries, stream_key, low, largest):
    longest = entries.shape.index(max(entries.shape))
    spots = []
    for shift in (0, 1):
        where = [jax.random.randint(jax.random.fold_in(stream_key, axis), (), 0, length) for axis, length in enumerate(entries.shape)]
        where[longest] = (where[longest] + shift) % entries.shape[longest]
        spots.append(tuple(where))
    return entries.at[spots[0]].set(low).at[spots[1]].set(largest)


def shard_levels(own_key, shape, cuts, smallest, top_value):
    loudness = 1.0
    for dim, shards_of in cuts:
        draws = jax.random.uniform(jax.random.fold_in(jax.random.fold_in(own_key, 6), dim), (shards_of,), jnp.float32, smallest / len(cuts), top_value / len(cuts))
        loudness = loudness * jnp.repeat(jnp.exp(draws), shape[dim] // shards_of).reshape((-1,) + (1,) * (len(shape) - 1 - dim))
    return loudness


def scatter_about(own_key, extent, width, reach, shards=(), kind=jnp.bfloat16):
    drawn = jax.random.normal(own_key, extent, jnp.float32) * width
    if len(shards) > 0:
        drawn = shard_levels(own_key, extent, shards, -0.22, 0.18) * drawn
    return jnp.clip(drawn, min=-reach, max=reach).astype(kind)


def setup_inputs(seed: int = 0) -> dict:
    key_list = jax.random.split(jax.random.key(seed), 12)
    noisy = draw_noisy(jax.random.fold_in(key_list[11], 71), 0)
    w_in = scatter_about(key_list[1], (C0, V), V ** -0.5, 3.0, (), jnp.float32)
    k_first = scatter_about(key_list[2], (3, 3, C0, C0), (9 * C0) ** -0.5, 0.25)
    w_down = scatter_about(key_list[3], (C1, C0), C0 ** -0.5, 0.75)
    k_coarse = scatter_about(key_list[4], (3, 3, C1, C1), (9 * C1) ** -0.5, 0.125)
    w_up = scatter_about(key_list[5], (C0, C1), C1 ** -0.5, 0.375)
    k_last = scatter_about(key_list[6], (3, 3, C0, C0), (9 * C0) ** -0.5, 0.25)
    w_out = scatter_about(key_list[7], (V, C0), C0 ** -0.5, 0.75)
    station_cell = set_ends(jax.random.randint(key_list[8], (BROWS, BCOLS, STA), 0, H_DEV * W_DEV), jax.random.fold_in(key_list[8], 1), 0, (H_DEV * W_DEV) - 1).astype(jnp.int32)
    station_count = set_ends(jax.random.randint(key_list[9], (BROWS, BCOLS, STA), 0, 4), jax.random.fold_in(key_list[9], 1), 0, 3).astype(jnp.int32)
    observed = scatter_about(key_list[10], (V, BROWS, BCOLS, STA), 1.0, 6.0, ((1, 64), (2, 4)), jnp.float32)
    return {"noisy": noisy, "w_in": w_in, "k_first": k_first, "w_down": w_down, "k_coarse": k_coarse, "w_up": w_up, "k_last": k_last, "w_out": w_out, "station_cell": station_cell, "station_count": station_count, "observed": observed}


def convolve(tensor, kernel):
    weights = jnp.transpose(kernel.astype(jnp.float32), (2, 3, 0, 1))
    result = lax.conv_general_dilated(tensor.astype(jnp.float32)[None], weights, (1, 1), "SAME", dimension_numbers=("NCHW", "OIHW", "NCHW"), precision=lax.Precision.HIGHEST)
    return result[0]


def reference(noisy, w_in, k_first, w_down, k_coarse, w_up, k_last, w_out, station_cell, station_count, observed):
    lifted = jnp.einsum("cv,vhw->chw", w_in, noisy, precision=lax.Precision.HIGHEST).astype(jnp.bfloat16)
    fine_one = (lifted.astype(jnp.float32) + jax.nn.silu(convolve(lifted, k_first))).astype(jnp.bfloat16)
    rows_all = fine_one.shape[1] // POOL
    cols_all = fine_one.shape[2] // POOL
    pooled = fine_one.astype(jnp.float32).reshape(C0, rows_all, POOL, cols_all, POOL).mean(axis=(2, 4)).astype(jnp.bfloat16)
    coarse_in = jnp.einsum("dc,chw->dhw", w_down.astype(jnp.float32), pooled.astype(jnp.float32)).astype(jnp.bfloat16)
    coarse_out = (coarse_in.astype(jnp.float32) + jax.nn.silu(convolve(coarse_in, k_coarse))).astype(jnp.bfloat16)
    raised = jnp.einsum("cd,dhw->chw", w_up.astype(jnp.float32), coarse_out.astype(jnp.float32))
    raised = jnp.broadcast_to(raised[:, :, None, :, None], (C0, rows_all, POOL, cols_all, POOL)).reshape(fine_one.shape)
    fine_two = (fine_one.astype(jnp.float32) + raised).astype(jnp.bfloat16)
    fine_three = (fine_two.astype(jnp.float32) + jax.nn.silu(convolve(fine_two, k_last))).astype(jnp.bfloat16)
    denoised = jnp.einsum("vc,chw->vhw", w_out.astype(jnp.float32), fine_three.astype(jnp.float32))
    grid_cols = denoised.shape[2]
    block_rows = jnp.arange(BROWS, dtype=jnp.int32)[:, None, None] * H_DEV
    block_cols = jnp.arange(BCOLS, dtype=jnp.int32)[None, :, None] * W_DEV
    row_index = block_rows + station_cell // W_DEV
    col_index = block_cols + station_cell % W_DEV
    flat_index = (row_index * grid_cols + col_index).astype(jnp.int32).reshape(-1)
    flat_field = denoised.reshape(V, -1)
    at_station = flat_field[:, flat_index]
    misfit = station_count.reshape(-1).astype(jnp.float32) * (observed.reshape(V, -1) - at_station)
    guide = jnp.zeros_like(flat_field).at[:, flat_index].add(misfit).reshape(denoised.shape)
    return noisy + 0.5 * (denoised - noisy) + 0.25 * guide
```

```python
import functools

import jax
import jax.numpy as jnp
from jax import lax
from jax.experimental import pallas as pl
from jax.experimental.pallas import tpu as pltpu
from jax.sharding import PartitionSpec as P

F32 = jnp.float32
BF16 = jnp.bfloat16
MESH = pl.DeviceIdType.MESH
NEAR = tuple((dr, dq) for dr in (-1, 0, 1) for dq in (-1, 0, 1) if (dr, dq) != (0, 0))
WIDE = tuple((dr, dq) for dr in (-2, -1, 0, 1, 2) for dq in (-1, 0, 1))
HB = 32
WB = 256
WE = 384
OWN = 9


def dot(a, b):
    return lax.dot_general(a, b, (((1,), (0,)), ((), ())), preferred_element_type=F32)


def dot_t(a, b):
    return lax.dot_general(a, b, (((1,), (1,)), ((), ())), preferred_element_type=F32)


def split2(x):
    high = x.astype(BF16)
    return high, (x - high.astype(F32)).astype(BF16)


def split3(x):
    high = x.astype(BF16)
    rest = x - high.astype(F32)
    middle = rest.astype(BF16)
    return high, middle, (rest - middle.astype(F32)).astype(BF16)


def kernel(
    n_rows,
    n_cols,
    n_ty,
    noisy_h, w_in_h, kf_h, wd_h, kc_h, wu_h, kl_h, wo_h, cell_h, count_h, obs_h,
    out_h,
    noisy_v, w_in_v, kf_v, wd_v, kc_v, wu_v, kl_v, wo_v, cell_v, count_v, obs_v,
    row_send, col_send, row_recv, col_recv, pool_send, pool_recv,
    ext, taps, taps_h, taps_l, a1, a2, w9, wo8, expand, fine, fine_l, fine_r, acc,
    station_a, station_b, fine_three, coarse, up_b, s_ref, raised_ref, out_v,
    in_sem, out_sem, near_send, near_recv, wide_send, wide_recv,
):
    row = lax.axis_index("grp") * n_ty + lax.axis_index("ty")
    col = lax.axis_index("tx")

    def device(dr, dq):
        r = lax.rem(row + dr + n_rows, n_rows)
        q = lax.rem(col + dq + n_cols, n_cols)
        return (r // n_ty, lax.rem(r, n_ty), q)

    def row_ok(dr):
        return jnp.logical_and(row + dr >= 0, row + dr < n_rows)

    def col_ok(dq):
        return jnp.logical_and(col + dq >= 0, col + dq < n_cols)

    pairs = (
        (noisy_h, noisy_v), (w_in_h, w_in_v), (kf_h, kf_v), (kl_h, kl_v), (wo_h, wo_v), (cell_h, cell_v),
        (count_h, count_v), (obs_h, obs_v), (wd_h, wd_v), (wu_h, wu_v), (kc_h, kc_v),
    )
    loads = [pltpu.make_async_copy(src, dst, in_sem.at[k]) for k, (src, dst) in enumerate(pairs)]
    for load in loads:
        load.start()

    barrier = pltpu.get_barrier_semaphore()
    for dr, dq in NEAR:
        pl.semaphore_signal(barrier, inc=1, device_id=device(dr, dq), device_id_type=MESH)

    loads[0].wait()
    for v in range(4):
        row_send[0, 2 * v : 2 * v + 2, :] = noisy_v[v, 0:2, :]
        row_send[1, 2 * v : 2 * v + 2, :] = noisy_v[v, HB - 2 : HB, :]
    first = jnp.concatenate([noisy_v[v, :, 0:128] for v in range(4)], axis=0)
    last = jnp.concatenate([noisy_v[v, :, 128:256] for v in range(4)], axis=0)
    col_send[0] = first.T[0:8, :]
    col_send[1] = last.T[120:128, :]

    pl.semaphore_wait(barrier, len(NEAR))
    near = []
    for k, (dr, dq) in enumerate(NEAR):
        if dq == 0:
            src = row_send.at[0 if dr < 0 else 1]
            dst = row_recv.at[1 if dr < 0 else 0]
        else:
            src = col_send.at[0 if dq < 0 else 1]
            dst = col_recv.at[1 if dq < 0 else 0, 1 - dr]
        back = NEAR.index((-dr, -dq))
        near.append(
            pltpu.make_async_remote_copy(
                src_ref=src, dst_ref=dst, send_sem=near_send.at[k], recv_sem=near_recv.at[back],
                device_id=device(dr, dq), device_id_type=MESH,
            )
        )
    for copy in near:
        copy.start()

    for load in loads[1:]:
        load.wait()
    w_tiled = dot_hi(w_in_v[...])
    lane = lax.broadcasted_iota(jnp.int32, (64, 128), 1)
    zero64 = jnp.zeros((64, 64), BF16)
    kf9 = jnp.concatenate([kf_v[p, q] for p in range(3) for q in range(3)], axis=1)
    for r in range(4):
        placed = []
        for p in range(3):
            for q in range(3):
                at = 12 * (r + p) + 4 * q
                placed.append(jnp.where(jnp.logical_and(lane >= at, lane < at + 4), w_tiled, 0.0))
        placed = jnp.concatenate(placed, axis=0)
        high, middle, low = split3(placed)
        conv = 0.5 * (dot(kf9, high) + dot(kf9, middle) + dot(kf9, low))
        at = 12 * (r + 1) + 4
        lift = jnp.where(jnp.logical_and(lane >= at, lane < at + 4), w_tiled, 0.0)
        high, low = split2(jnp.concatenate([conv, lift], axis=0))
        a1[r, :, 0:80] = high[:, 0:80]
        a1[r, :, 80:160] = high[:, 0:80]
        a1[r, :, 160:240] = low[:, 0:80]
    half = [[(kl_v[p, q].astype(F32) * 0.5).astype(BF16) for q in range(3)] for p in range(3)]
    for q in range(3):
        upper = jnp.concatenate([half[0][q], half[1][q], half[2][q], zero64], axis=1)
        lower = jnp.concatenate([zero64, half[0][q], half[1][q], half[2][q]], axis=1)
        a2[q] = jnp.concatenate([upper, lower], axis=0)
    w9[...] = jnp.concatenate([half[p][q] for p in range(3) for q in range(3)], axis=1)
    pick = (lax.broadcasted_iota(jnp.int32, (32, 4), 0) // 8 == lax.broadcasted_iota(jnp.int32, (32, 4), 1))
    spread = dot(pick.astype(BF16), wo_v[...])
    spread = jnp.concatenate([spread] * 8, axis=1)
    same = lax.broadcasted_iota(jnp.int32, (32, 512), 0) % 8 == lax.broadcasted_iota(jnp.int32, (32, 512), 1) // 64
    wo8[...] = jnp.where(same, spread, 0.0).astype(BF16)
    cells = lax.broadcasted_iota(jnp.int32, (72, WB), 0)
    pixel = lax.broadcasted_iota(jnp.int32, (72, WB), 1)
    for rho in range(3):
        for q in range(3):
            want = rho * 24 + 7 + (pixel + (32 + q - 1)) // 32
            expand[rho * 3 + q] = (cells == want).astype(F32).astype(BF16)

    cell = cell_v[0]
    count = count_v[0].astype(F32)
    at_row = (lax.broadcasted_iota(jnp.int32, (HB, 128), 0) == cell // WB).astype(F32)
    at_col = (lax.broadcasted_iota(jnp.int32, (WB, 128), 0) == cell % WB).astype(F32).astype(BF16)
    reports = [at_row * (count * obs_v[v, 0]) for v in range(4)] + [at_row * count]
    parts = split3(jnp.concatenate(reports, axis=0))
    sums = dot_t(parts[0], at_col) + dot_t(parts[1], at_col) + dot_t(parts[2], at_col)
    for v in range(4):
        station_a[v] = 0.5 * noisy_v[v] + 0.25 * sums[HB * v : HB * (v + 1)]
    station_b[...] = 0.5 - 0.25 * sums[HB * 4 :]

    for copy in near:
        copy.wait()
    ext[...] = jnp.zeros_like(ext)
    for v in range(4):
        ext[v, OWN : OWN + HB, 0:WB] = noisy_v[v]
        ext[v, OWN - 2 : OWN, 0:WB] = jnp.where(row_ok(-1), row_recv[0, 2 * v : 2 * v + 2, :], 0.0)
        ext[v, OWN + HB : OWN + HB + 2, 0:WB] = jnp.where(row_ok(1), row_recv[1, 2 * v : 2 * v + 2, :], 0.0)
    for k in range(3):
        right = jnp.where(jnp.logical_and(row_ok(k - 1), col_ok(1)), col_recv[1, k], 0.0)
        left = jnp.where(jnp.logical_and(row_ok(k - 1), col_ok(-1)), col_recv[0, k], 0.0)
        side = jnp.concatenate([right, jnp.zeros((112, 128), F32), left], axis=0).T
        for v in range(4):
            if k == 0:
                ext[v, OWN - 2 : OWN, WB:WE] = side[HB * v + HB - 2 : HB * v + HB]
            elif k == 1:
                ext[v, OWN : OWN + HB, WB:WE] = side[HB * v : HB * (v + 1)]
            else:
                ext[v, OWN + HB : OWN + HB + 2, WB:WE] = side[HB * v : HB * v + 2]
    for v in range(4):
        for t in range(3):
            here = ext[v, :, 128 * t : 128 * t + 128]
            before = ext[v, :, 128 * ((t + 2) % 3) : 128 * ((t + 2) % 3) + 128]
            after = ext[v, :, 128 * ((t + 1) % 3) : 128 * ((t + 1) % 3) + 128]
            spot = lax.broadcasted_iota(jnp.int32, here.shape, 1)
            shifted = (
                jnp.where(spot < 1, pltpu.roll(before, 1, 1), pltpu.roll(here, 1, 1)),
                here,
                jnp.where(spot < 127, pltpu.roll(here, 127, 1), pltpu.roll(after, 127, 1)),
            )
            for q in range(3):
                taps[t, pl.ds(4 * q + v, 48, stride=12), :] = shifted[q]
    for t in range(3):
        high, low = split2(taps[t])
        taps_h[:, 128 * t : 128 * t + 128] = high
        taps_l[:, 128 * t : 128 * t + 128] = low

    def window(at, lanes):
        high = taps_h[pl.ds(at, 80), lanes]
        return jnp.concatenate([high, taps_l[pl.ds(at, 80), lanes], high], axis=0)

    def gated(both):
        h = both[0:64]
        return both[64:128] + (h + h * jnp.tanh(h))

    def own_rows(g, pool):
        rhs = window(pl.multiple_of(96 + 48 * g, 16), slice(0, WB))
        for r in range(4):
            value = gated(dot(a1[r], rhs))
            at = pl.multiple_of((4 * g + r + 1) * 64, 64)
            fine[pl.ds(at, 64), 0:WB] = value.astype(BF16)
            pool = pool + value
        return pool

    pool = lax.fori_loop(0, 8, own_rows, jnp.zeros((64, WB), F32))
    into = lax.broadcasted_iota(jnp.int32, (8, WB), 1) // 32 == lax.broadcasted_iota(jnp.int32, (8, WB), 0)
    into = into.astype(F32).astype(BF16)
    high, low = split2(jnp.concatenate([pool, jnp.zeros((64, WB), F32)], axis=0))
    pooled = (dot_t(into, high) + dot_t(into, low)) * (1.0 / 1024.0)
    pool_send[...] = pooled
    wide = []
    for k, (dr, dq) in enumerate(WIDE):
        if (dr, dq) == (0, 0):
            continue
        back = WIDE.index((-dr, -dq))
        wide.append(
            pltpu.make_async_remote_copy(
                src_ref=pool_send, dst_ref=pool_recv.at[back], send_sem=wide_send.at[k],
                recv_sem=wide_recv.at[back], device_id=device(dr, dq), device_id_type=MESH,
            )
        )
    for copy in wide:
        copy.start()
    pool_recv[WIDE.index((0, 0))] = pooled

    side_lane = lax.broadcasted_iota(jnp.int32, (64, 128), 1)
    right_gate = jnp.where(col_ok(1), 1.0, 0.0)
    left_gate = jnp.where(col_ok(-1), 1.0, 0.0)
    side_gate = jnp.where(side_lane < 64, right_gate, left_gate)

    def side_rows(g, carry):
        rhs = jnp.concatenate(
            [
                window(pl.multiple_of(96 + 96 * g, 16), slice(WB, WE)),
                window(pl.multiple_of(144 + 96 * g, 16), slice(WB, WE)),
            ],
            axis=1,
        )
        for r in range(4):
            value = gated(dot(a1[r], rhs))
            for k in range(2):
                at = pl.multiple_of((8 * g + 4 * k + r + 1) * 64, 64)
                fine[pl.ds(at, 64), WB:WE] = (value[:, 128 * k : 128 * k + 128] * side_gate).astype(BF16)
        return carry

    lax.fori_loop(0, 4, side_rows, 0)
    for at, r, e, gate in ((48, 3, 0, row_ok(-1)), (480, 0, 33, row_ok(1))):
        gate = jnp.where(gate, 1.0, 0.0)
        value = gated(dot(a1[r], window(at, slice(0, WB)))) * gate
        fine[e * 64 : e * 64 + 64, 0:WB] = value.astype(BF16)
        value = gated(dot(a1[r], window(at, slice(WB, WE)))) * side_gate * gate
        fine[e * 64 : e * 64 + 64, WB:WE] = value.astype(BF16)

    def shift_rows(e, carry):
        at = pl.multiple_of(e * 64, 64)
        tile = [fine[pl.ds(at, 64), 128 * t : 128 * t + 128] for t in range(3)]
        spot = lax.broadcasted_iota(jnp.int32, (64, 128), 1)
        tile = [x.astype(F32) for x in tile]
        up = [pltpu.roll(x, 1, 1) for x in tile]
        down = [pltpu.roll(x, 127, 1) for x in tile]
        fine_l[pl.ds(at, 64), 0:128] = jnp.where(spot < 1, up[2], up[0]).astype(BF16)
        fine_l[pl.ds(at, 64), 128:256] = jnp.where(spot < 1, up[0], up[1]).astype(BF16)
        fine_r[pl.ds(at, 64), 0:128] = jnp.where(spot < 127, down[0], down[1]).astype(BF16)
        fine_r[pl.ds(at, 64), 128:256] = jnp.where(spot < 127, down[1], down[2]).astype(BF16)
        return carry

    lax.fori_loop(0, HB + 2, shift_rows, 0)

    def last_rows(k, carry):
        at = pl.multiple_of(k * 128, 128)
        total = dot(a2[0], fine_l[pl.ds(at, 256), :])
        total += dot(a2[1], fine[pl.ds(at, 256), 0:WB])
        total += dot(a2[2], fine_r[pl.ds(at, 256), :])
        acc[pl.ds(at, 128), :] = total
        return carry

    lax.fori_loop(0, 16, last_rows, 0)

    for copy in wide:
        copy.wait()
    cells = []
    for k, (dr, dq) in enumerate(WIDE):
        cells.append(jnp.where(jnp.logical_and(row_ok(dr), col_ok(dq)), pool_recv[k], 0.0))
    cells = jnp.concatenate(cells, axis=0).astype(BF16)
    entering = dot_t(cells[:, 0:64], wd_v[...])
    coarse[0:8] = jnp.zeros((8, 256), F32)
    coarse[128:136] = jnp.zeros((8, 256), F32)
    coarse[8:128] = entering.astype(BF16).astype(F32)
    total = jnp.zeros((72, 256), F32)
    for p in range(3):
        for q in range(3):
            at = 8 + 24 * p + q - 1
            total += dot_t(coarse[at : at + 72].astype(BF16), kc_v[p, q])
    half_total = 0.5 * total
    leaving = coarse[32:104] + (half_total + half_total * jnp.tanh(half_total))
    blocks = []
    for k, (dr, dq) in enumerate(WIDE[3:12]):
        block = leaving[8 * k : 8 * k + 8]
        blocks.append(jnp.where(jnp.logical_and(row_ok(dr), col_ok(dq)), block, 0.0))
    leaving = jnp.concatenate(blocks, axis=0).astype(BF16)
    high, low = split2(dot_t(wu_v[...], leaving))
    for k in range(9):
        wide_up = dot(high, expand[k])
        up_b[k] = wide_up.astype(BF16)
        if k == 4:
            raised_ref[...] = wide_up + dot(low, expand[k])
    for edge, rhos in enumerate(((0, 1, 1), (1, 1, 1), (1, 1, 2))):
        rhs = jnp.concatenate([up_b[rhos[p] * 3 + q] for p in range(3) for q in range(3)], axis=0)
        s_ref[edge] = dot(w9[...], rhs)

    def finish(i, edge):
        at = i * 64 if isinstance(i, int) else pl.multiple_of(i * 64, 64)
        h = acc[pl.ds(at, 64), :] + s_ref[edge]
        one = fine[pl.ds(at + 64, 64), 0:WB].astype(F32)
        value = one + raised_ref[...] + (h + h * jnp.tanh(h))
        fine_three[pl.ds(at, 64), :] = value.astype(BF16)

    def finish_middle(i, carry):
        finish(i, 1)
        return carry

    finish(0, 0)
    finish(HB - 1, 2)
    lax.fori_loop(1, HB - 1, finish_middle, 0)
    for g in range(4):
        denoised = dot(wo8[...], fine_three[512 * g : 512 * g + 512, :])
        for v in range(4):
            rows = slice(8 * g, 8 * g + 8)
            out_v[v, rows, :] = station_a[v, rows, :] + station_b[rows, :] * denoised[8 * v : 8 * v + 8]
    store = pltpu.make_async_copy(out_v, out_h, out_sem)
    store.start()
    store.wait()


def dot_hi(w_in):
    place = lax.broadcasted_iota(jnp.int32, (4, 128), 1) % 4 == lax.broadcasted_iota(jnp.int32, (4, 128), 0)
    place = place.astype(F32).astype(BF16)
    high, middle, low = split3(w_in)
    return (dot(high, place) + dot(middle, place)) + dot(low, place)


def solution(mesh):
    n_ty = mesh.shape["ty"]
    n_rows = mesh.shape["grp"] * n_ty
    n_cols = mesh.shape["tx"]

    def on_device(noisy, w_in, kf, wd, kc, wu, kl, wo, cell, count, obs):
        obs = obs.reshape(4, 1, 128)
        cell = cell.reshape(1, 1, 128)
        count = count.reshape(1, 1, 128)
        args = (noisy, w_in, kf, wd, kc, wu, kl, wo, cell, count, obs)
        vmem = pltpu.VMEM
        return pl.pallas_call(
            functools.partial(kernel, n_rows, n_cols, n_ty),
            out_shape=jax.ShapeDtypeStruct(noisy.shape, noisy.dtype),
            in_specs=[pl.BlockSpec(memory_space=pl.ANY)] * 11,
            out_specs=pl.BlockSpec(memory_space=pl.ANY),
            scratch_shapes=[vmem(x.shape, x.dtype) for x in args]
            + [
                vmem((2, 8, WB), F32),
                vmem((2, 8, 128), F32),
                vmem((2, 8, WB), F32),
                vmem((2, 3, 8, 128), F32),
                vmem((8, 128), F32),
                vmem((15, 8, 128), F32),
                vmem((4, 48, WE), F32),
                vmem((3, 576, 128), F32),
                vmem((576, WE), BF16),
                vmem((576, WE), BF16),
                vmem((4, 128, 240), BF16),
                vmem((3, 128, 256), BF16),
                vmem((64, 576), BF16),
                vmem((32, 512), BF16),
                vmem((9, 72, WB), BF16),
                vmem((34 * 64, WE), BF16),
                vmem((34 * 64, WB), BF16),
                vmem((34 * 64, WB), BF16),
                vmem((HB * 64, WB), F32),
                vmem((4, HB, WB), F32),
                vmem((HB, WB), F32),
                vmem((HB * 64, WB), BF16),
                vmem((136, 256), F32),
                vmem((9, 64, WB), BF16),
                vmem((3, 64, WB), F32),
                vmem((64, WB), F32),
                vmem((4, HB, WB), F32),
                pltpu.SemaphoreType.DMA((11,)),
                pltpu.SemaphoreType.DMA,
                pltpu.SemaphoreType.DMA((8,)),
                pltpu.SemaphoreType.DMA((8,)),
                pltpu.SemaphoreType.DMA((15,)),
                pltpu.SemaphoreType.DMA((15,)),
            ],
            compiler_params=pltpu.CompilerParams(
                collective_id=0, has_side_effects=True, vmem_limit_bytes=40 * 1024 * 1024
            ),
        )(*args)

    return jax.shard_map(
        on_device,
        mesh=mesh,
        in_specs=(
            P(None, ("grp", "ty"), "tx"),
            P(),
            P(),
            P(),
            P(),
            P(),
            P(),
            P(),
            P(("grp", "ty"), "tx", None),
            P(("grp", "ty"), "tx", None),
            P(None, ("grp", "ty"), "tx", None),
        ),
        out_specs=P(None, ("grp", "ty"), "tx"),
        check_vma=False,
    )
```

```python
import functools

import jax
import jax.numpy as jnp
from jax import lax
from jax.experimental import pallas as pl
from jax.experimental.pallas import tpu as pltpu
from jax.sharding import PartitionSpec as P

F32 = jnp.float32
BF16 = jnp.bfloat16
MESH = pl.DeviceIdType.MESH
NEAR = tuple((dr, dq) for dr in (-1, 0, 1) for dq in (-1, 0, 1) if (dr, dq) != (0, 0))
WIDE = tuple((dr, dq) for dr in (-2, -1, 0, 1, 2) for dq in (-1, 0, 1))
HB = 32
WB = 256
WE = 384
OWN = 9


def dot(a, b):
    return lax.dot_general(a, b, (((1,), (0,)), ((), ())), preferred_element_type=F32)


def dot_t(a, b):
    return lax.dot_general(a, b, (((1,), (1,)), ((), ())), preferred_element_type=F32)


def split2(x):
    high = x.astype(BF16)
    return high, (x - high.astype(F32)).astype(BF16)


def split3(x):
    high = x.astype(BF16)
    rest = x - high.astype(F32)
    middle = rest.astype(BF16)
    return high, middle, (rest - middle.astype(F32)).astype(BF16)


def kernel(
    n_rows,
    n_cols,
    n_ty,
    noisy_h, w_in_h, kf_h, wd_h, kc_h, wu_h, kl_h, wo_h, cell_h, count_h, obs_h,
    out_h,
    noisy_v, w_in_v, kf_v, wd_v, kc_v, wu_v, kl_v, wo_v, cell_v, count_v, obs_v,
    row_send, col_send, row_recv, col_recv, pool_send, pool_recv,
    ext, taps, taps_h, taps_l, a1, a2, w9, wo8, expand, fine, fine_l, fine_r, acc,
    station_a, station_b, fine_three, coarse, up_b, s_ref, raised_ref, out_v,
    in_sem, out_sem, near_send, near_recv, wide_send, wide_recv,
):
    row = lax.axis_index("grp") * n_ty + lax.axis_index("ty")
    col = lax.axis_index("tx")

    def device(dr, dq):
        r = lax.rem(row + dr + n_rows, n_rows)
        q = lax.rem(col + dq + n_cols, n_cols)
        return (r // n_ty, lax.rem(r, n_ty), q)

    def row_ok(dr):
        return jnp.logical_and(row + dr >= 0, row + dr < n_rows)

    def col_ok(dq):
        return jnp.logical_and(col + dq >= 0, col + dq < n_cols)

    pairs = (
        (noisy_h, noisy_v), (w_in_h, w_in_v), (kf_h, kf_v), (kl_h, kl_v), (wo_h, wo_v), (cell_h, cell_v),
        (count_h, count_v), (obs_h, obs_v), (wd_h, wd_v), (wu_h, wu_v), (kc_h, kc_v),
    )
    loads = [pltpu.make_async_copy(src, dst, in_sem.at[k]) for k, (src, dst) in enumerate(pairs)]
    for load in loads:
        load.start()

    barrier = pltpu.get_barrier_semaphore()
    for dr, dq in NEAR:
        pl.semaphore_signal(barrier, inc=1, device_id=device(dr, dq), device_id_type=MESH)

    loads[0].wait()
    for v in range(4):
        row_send[0, 2 * v : 2 * v + 2, :] = noisy_v[v, 0:2, :]
        row_send[1, 2 * v : 2 * v + 2, :] = noisy_v[v, HB - 2 : HB, :]
    first = jnp.concatenate([noisy_v[v, :, 0:128] for v in range(4)], axis=0)
    last = jnp.concatenate([noisy_v[v, :, 128:256] for v in range(4)], axis=0)
    col_send[0] = first.T[0:8, :]
    col_send[1] = last.T[120:128, :]

    pl.semaphore_wait(barrier, len(NEAR))
    near = []
    for k, (dr, dq) in enumerate(NEAR):
        if dq == 0:
            src = row_send.at[0 if dr < 0 else 1]
            dst = row_recv.at[1 if dr < 0 else 0]
        else:
            src = col_send.at[0 if dq < 0 else 1]
            dst = col_recv.at[1 if dq < 0 else 0, 1 - dr]
        back = NEAR.index((-dr, -dq))
        near.append(
            pltpu.make_async_remote_copy(
                src_ref=src, dst_ref=dst, send_sem=near_send.at[k], recv_sem=near_recv.at[back],
                device_id=device(dr, dq), device_id_type=MESH,
            )
        )
    for copy in near:
        copy.start()

    for load in loads[1:]:
        load.wait()
    w_tiled = dot_hi(w_in_v[...].T)
    lane = lax.broadcasted_iota(jnp.int32, (64, 128), 1)
    zero64 = jnp.zeros((64, 64), BF16)
    kf9 = jnp.concatenate([kf_v[p, q] for p in range(3) for q in range(3)], axis=1)
    for r in range(4):
        placed = []
        for p in range(3):
            for q in range(3):
                at = 12 * (r + p) + 4 * q
                placed.append(jnp.where(jnp.logical_and(lane >= at, lane < at + 4), w_tiled, 0.0))
        placed = jnp.concatenate(placed, axis=0)
        high, middle, low = split3(placed)
        conv = 0.5 * (dot(kf9, high) + dot(kf9, middle) + dot(kf9, low))
        at = 12 * (r + 1) + 4
        lift = jnp.where(jnp.logical_and(lane >= at, lane < at + 4), w_tiled, 0.0)
        high, low = split2(jnp.concatenate([conv, lift], axis=0))
        a1[r, :, 0:80] = high[:, 0:80]
        a1[r, :, 80:160] = high[:, 0:80]
        a1[r, :, 160:240] = low[:, 0:80]
    half = [[(kl_v[p, q].astype(F32) * 0.5).astype(BF16) for q in range(3)] for p in range(3)]
    for q in range(3):
        upper = jnp.concatenate([half[0][q], half[1][q], half[2][q], zero64], axis=1)
        lower = jnp.concatenate([zero64, half[0][q], half[1][q], half[2][q]], axis=1)
        a2[q] = jnp.concatenate([upper, lower], axis=0)
    w9[...] = jnp.concatenate([half[p][q] for p in range(3) for q in range(3)], axis=1)
    pick = (lax.broadcasted_iota(jnp.int32, (32, 4), 0) // 8 == lax.broadcasted_iota(jnp.int32, (32, 4), 1))
    spread = dot(pick.astype(BF16), wo_v[...])
    spread = jnp.concatenate([spread] * 8, axis=1)
    same = lax.broadcasted_iota(jnp.int32, (32, 512), 0) % 8 == lax.broadcasted_iota(jnp.int32, (32, 512), 1) // 64
    wo8[...] = jnp.where(same, spread, 0.0).astype(BF16)
    cells = lax.broadcasted_iota(jnp.int32, (72, WB), 0)
    pixel = lax.broadcasted_iota(jnp.int32, (72, WB), 1)
    for rho in range(3):
        for q in range(3):
            want = rho * 24 + 7 + (pixel + (32 + q - 1)) // 32
            expand[rho * 3 + q] = (cells == want).astype(F32).astype(BF16)

    cell = cell_v[0]
    count = count_v[0].astype(F32)
    at_row = (lax.broadcasted_iota(jnp.int32, (HB, 128), 0) == cell // WB).astype(F32)
    at_col = (lax.broadcasted_iota(jnp.int32, (WB, 128), 0) == cell % WB).astype(F32).astype(BF16)
    reports = [at_row * (count * obs_v[v, 0]) for v in range(4)] + [at_row * count]
    parts = split3(jnp.concatenate(reports, axis=0))
    sums = dot_t(parts[0], at_col) + dot_t(parts[1], at_col) + dot_t(parts[2], at_col)
    for v in range(4):
        station_a[v] = 0.5 * noisy_v[v] + 0.25 * sums[HB * v : HB * (v + 1)]
    station_b[...] = 0.5 - 0.25 * sums[HB * 4 :]

    for copy in near:
        copy.wait()
    ext[...] = jnp.zeros_like(ext)
    for v in range(4):
        ext[v, OWN : OWN + HB, 0:WB] = noisy_v[v]
        ext[v, OWN - 2 : OWN, 0:WB] = jnp.where(row_ok(-1), row_recv[0, 2 * v : 2 * v + 2, :], 0.0)
        ext[v, OWN + HB : OWN + HB + 2, 0:WB] = jnp.where(row_ok(1), row_recv[1, 2 * v : 2 * v + 2, :], 0.0)
    for k in range(3):
        right = jnp.where(jnp.logical_and(row_ok(k - 1), col_ok(1)), col_recv[1, k], 0.0)
        left = jnp.where(jnp.logical_and(row_ok(k - 1), col_ok(-1)), col_recv[0, k], 0.0)
        side = jnp.concatenate([right, jnp.zeros((112, 128), F32), left], axis=0).T
        for v in range(4):
            if k == 0:
                ext[v, OWN - 2 : OWN, WB:WE] = side[HB * v + HB - 2 : HB * v + HB]
            elif k == 1:
                ext[v, OWN : OWN + HB, WB:WE] = side[HB * v : HB * (v + 1)]
            else:
                ext[v, OWN + HB : OWN + HB + 2, WB:WE] = side[HB * v : HB * v + 2]
    for v in range(4):
        for t in range(3):
            here = ext[v, :, 128 * t : 128 * t + 128]
            before = ext[v, :, 128 * ((t + 2) % 3) : 128 * ((t + 2) % 3) + 128]
            after = ext[v, :, 128 * ((t + 1) % 3) : 128 * ((t + 1) % 3) + 128]
            spot = lax.broadcasted_iota(jnp.int32, here.shape, 1)
            shifted = (
                jnp.where(spot < 1, pltpu.roll(before, 1, 1), pltpu.roll(here, 1, 1)),
                here,
                jnp.where(spot < 127, pltpu.roll(here, 127, 1), pltpu.roll(after, 127, 1)),
            )
            for q in range(3):
                taps[t, pl.ds(4 * q + v, 48, stride=12), :] = shifted[q]
    for t in range(3):
        high, low = split2(taps[t])
        taps_h[:, 128 * t : 128 * t + 128] = high
        taps_l[:, 128 * t : 128 * t + 128] = low

    def window(at, lanes):
        high = taps_h[pl.ds(at, 80), lanes]
        return jnp.concatenate([high, taps_l[pl.ds(at, 80), lanes], high], axis=0)

    def gated(both):
        h = both[0:64]
        return both[64:128] + (h + h * jnp.tanh(h))

    def own_rows(g, pool):
        rhs = window(pl.multiple_of(96 + 48 * g, 16), slice(0, WB))
        for r in range(4):
            value = gated(dot(a1[r], rhs))
            at = pl.multiple_of((4 * g + r + 1) * 64, 64)
            fine[pl.ds(at, 64), 0:WB] = value.astype(BF16)
            pool = pool + value
        return pool

    pool = lax.fori_loop(0, 8, own_rows, jnp.zeros((64, WB), F32), unroll=True)
    into = lax.broadcasted_iota(jnp.int32, (8, WB), 1) // 32 == lax.broadcasted_iota(jnp.int32, (8, WB), 0)
    into = into.astype(F32).astype(BF16)
    high, low = split2(jnp.concatenate([pool, jnp.zeros((64, WB), F32)], axis=0))
    pooled = (dot_t(into, high) + dot_t(into, low)) * (1.0 / 1024.0)
    pool_send[...] = pooled
    wide = []
    for k, (dr, dq) in enumerate(WIDE):
        if (dr, dq) == (0, 0):
            continue
        back = WIDE.index((-dr, -dq))
        wide.append(
            pltpu.make_async_remote_copy(
                src_ref=pool_send, dst_ref=pool_recv.at[back], send_sem=wide_send.at[k],
                recv_sem=wide_recv.at[back], device_id=device(dr, dq), device_id_type=MESH,
            )
        )
    for copy in wide:
        copy.start()
    pool_recv[WIDE.index((0, 0))] = pooled

    side_lane = lax.broadcasted_iota(jnp.int32, (64, 128), 1)
    right_gate = jnp.where(col_ok(1), 1.0, 0.0)
    left_gate = jnp.where(col_ok(-1), 1.0, 0.0)
    side_gate = jnp.where(side_lane < 64, right_gate, left_gate)

    def side_rows(g, carry):
        rhs = jnp.concatenate(
            [
                window(pl.multiple_of(96 + 96 * g, 16), slice(WB, WE)),
                window(pl.multiple_of(144 + 96 * g, 16), slice(WB, WE)),
            ],
            axis=1,
        )
        for r in range(4):
            value = gated(dot(a1[r], rhs))
            for k in range(2):
                at = pl.multiple_of((8 * g + 4 * k + r + 1) * 64, 64)
                fine[pl.ds(at, 64), WB:WE] = (value[:, 128 * k : 128 * k + 128] * side_gate).astype(BF16)
        return carry

    lax.fori_loop(0, 4, side_rows, 0, unroll=True)
    for at, r, e, gate in ((48, 3, 0, row_ok(-1)), (480, 0, 33, row_ok(1))):
        gate = jnp.where(gate, 1.0, 0.0)
        value = gated(dot(a1[r], window(at, slice(0, WB)))) * gate
        fine[e * 64 : e * 64 + 64, 0:WB] = value.astype(BF16)
        value = gated(dot(a1[r], window(at, slice(WB, WE)))) * side_gate * gate
        fine[e * 64 : e * 64 + 64, WB:WE] = value.astype(BF16)

    def shift_rows(e, carry):
        at = pl.multiple_of(e * 64, 64)
        tile = [fine[pl.ds(at, 64), 128 * t : 128 * t + 128] for t in range(3)]
        spot = lax.broadcasted_iota(jnp.int32, (64, 128), 1)
        tile = [x.astype(F32) for x in tile]
        up = [pltpu.roll(x, 1, 1) for x in tile]
        down = [pltpu.roll(x, 127, 1) for x in tile]
        fine_l[pl.ds(at, 64), 0:128] = jnp.where(spot < 1, up[2], up[0]).astype(BF16)
        fine_l[pl.ds(at, 64), 128:256] = jnp.where(spot < 1, up[0], up[1]).astype(BF16)
        fine_r[pl.ds(at, 64), 0:128] = jnp.where(spot < 127, down[0], down[1]).astype(BF16)
        fine_r[pl.ds(at, 64), 128:256] = jnp.where(spot < 127, down[1], down[2]).astype(BF16)
        return carry

    lax.fori_loop(0, HB + 2, shift_rows, 0, unroll=True)

    def last_rows(k, carry):
        at = pl.multiple_of(k * 128, 128)
        total = dot(a2[0], fine_l[pl.ds(at, 256), :])
        total += dot(a2[1], fine[pl.ds(at, 256), 0:WB])
        total += dot(a2[2], fine_r[pl.ds(at, 256), :])
        acc[pl.ds(at, 128), :] = total
        return carry

    lax.fori_loop(0, 16, last_rows, 0, unroll=True)

    for copy in wide:
        copy.wait()
    cells = []
    for k, (dr, dq) in enumerate(WIDE):
        cells.append(jnp.where(jnp.logical_and(row_ok(dr), col_ok(dq)), pool_recv[k], 0.0))
    cells = jnp.concatenate(cells, axis=0).astype(BF16)
    entering = dot(cells[:, 0:64], wd_v[...])
    coarse[0:8] = jnp.zeros((8, 256), F32)
    coarse[128:136] = jnp.zeros((8, 256), F32)
    coarse[8:128] = entering.astype(BF16).astype(F32)
    total = jnp.zeros((72, 256), F32)
    for p in range(3):
        for q in range(3):
            at = 8 + 24 * p + q - 1
            total += dot_t(coarse[at : at + 72].astype(BF16), kc_v[p, q])
    half_total = 0.5 * total
    leaving = coarse[32:104] + (half_total + half_total * jnp.tanh(half_total))
    blocks = []
    for k, (dr, dq) in enumerate(WIDE[3:12]):
        block = leaving[8 * k : 8 * k + 8]
        blocks.append(jnp.where(jnp.logical_and(row_ok(dr), col_ok(dq)), block, 0.0))
    leaving = jnp.concatenate(blocks, axis=0).astype(BF16)
    high, low = split2(dot_t(wu_v[...], leaving))
    for k in range(9):
        wide_up = dot(high, expand[k])
        up_b[k] = wide_up.astype(BF16)
        if k == 4:
            raised_ref[...] = wide_up + dot(low, expand[k])
    for edge, rhos in enumerate(((0, 1, 1), (1, 1, 1), (1, 1, 2))):
        rhs = jnp.concatenate([up_b[rhos[p] * 3 + q] for p in range(3) for q in range(3)], axis=0)
        s_ref[edge] = dot(w9[...], rhs)

    def finish(i, edge):
        at = i * 64 if isinstance(i, int) else pl.multiple_of(i * 64, 64)
        h = acc[pl.ds(at, 64), :] + s_ref[edge]
        one = fine[pl.ds(at + 64, 64), 0:WB].astype(F32)
        value = one + raised_ref[...] + (h + h * jnp.tanh(h))
        fine_three[pl.ds(at, 64), :] = value.astype(BF16)

    def finish_middle(i, carry):
        finish(i, 1)
        return carry

    finish(0, 0)
    finish(HB - 1, 2)
    lax.fori_loop(1, HB - 1, finish_middle, 0, unroll=True)
    for g in range(4):
        denoised = dot(wo8[...], fine_three[512 * g : 512 * g + 512, :])
        for v in range(4):
            rows = slice(8 * g, 8 * g + 8)
            out_v[v, rows, :] = station_a[v, rows, :] + station_b[rows, :] * denoised[8 * v : 8 * v + 8]
    store = pltpu.make_async_copy(out_v, out_h, out_sem)
    store.start()
    store.wait()


def dot_hi(w_in):
    place = lax.broadcasted_iota(jnp.int32, (4, 128), 1) % 4 == lax.broadcasted_iota(jnp.int32, (4, 128), 0)
    place = place.astype(F32).astype(BF16)
    high, middle, low = split3(w_in)
    return (dot(high, place) + dot(middle, place)) + dot(low, place)


def solution(mesh):
    n_ty = mesh.shape["ty"]
    n_rows = mesh.shape["grp"] * n_ty
    n_cols = mesh.shape["tx"]

    def on_device(noisy, w_in, kf, wd, kc, wu, kl, wo, cell, count, obs):
        w_in, wd = w_in.T, wd.T
        obs = obs.reshape(4, 1, 128)
        cell = cell.reshape(1, 1, 128)
        count = count.reshape(1, 1, 128)
        args = (noisy, w_in, kf, wd, kc, wu, kl, wo, cell, count, obs)
        vmem = pltpu.VMEM
        return pl.pallas_call(
            functools.partial(kernel, n_rows, n_cols, n_ty),
            out_shape=jax.ShapeDtypeStruct(noisy.shape, noisy.dtype),
            in_specs=[pl.BlockSpec(memory_space=pltpu.HBM)] * 11,
            out_specs=pl.BlockSpec(memory_space=pl.ANY),
            scratch_shapes=[vmem(x.shape, x.dtype) for x in args]
            + [
                vmem((2, 8, WB), F32),
                vmem((2, 8, 128), F32),
                vmem((2, 8, WB), F32),
                vmem((2, 3, 8, 128), F32),
                vmem((8, 128), F32),
                vmem((15, 8, 128), F32),
                vmem((4, 48, WE), F32),
                vmem((3, 576, 128), F32),
                vmem((576, WE), BF16),
                vmem((576, WE), BF16),
                vmem((4, 128, 240), BF16),
                vmem((3, 128, 256), BF16),
                vmem((64, 576), BF16),
                vmem((32, 512), BF16),
                vmem((9, 72, WB), BF16),
                vmem((34 * 64, WE), BF16),
                vmem((34 * 64, WB), BF16),
                vmem((34 * 64, WB), BF16),
                vmem((HB * 64, WB), F32),
                vmem((4, HB, WB), F32),
                vmem((HB, WB), F32),
                vmem((HB * 64, WB), BF16),
                vmem((136, 256), F32),
                vmem((9, 64, WB), BF16),
                vmem((3, 64, WB), F32),
                vmem((64, WB), F32),
                vmem((4, HB, WB), F32),
                pltpu.SemaphoreType.DMA((11,)),
                pltpu.SemaphoreType.DMA,
                pltpu.SemaphoreType.DMA((8,)),
                pltpu.SemaphoreType.DMA((8,)),
                pltpu.SemaphoreType.DMA((15,)),
                pltpu.SemaphoreType.DMA((15,)),
            ],
            compiler_params=pltpu.CompilerParams(
                collective_id=0, has_side_effects=True, vmem_limit_bytes=67043328
            ),
        )(*args)

    return jax.shard_map(
        on_device,
        mesh=mesh,
        in_specs=(
            P(None, ("grp", "ty"), "tx"),
            P(),
            P(),
            P(),
            P(),
            P(),
            P(),
            P(),
            P(("grp", "ty"), "tx", None),
            P(("grp", "ty"), "tx", None),
            P(None, ("grp", "ty"), "tx", None),
        ),
        out_specs=P(None, ("grp", "ty"), "tx"),
        check_vma=False,
    )
```

```python
import functools

import jax
import jax.numpy as jnp
from jax import lax
from jax.experimental import pallas as pl
from jax.experimental.pallas import tpu as pltpu
from jax.sharding import PartitionSpec as P

F32 = jnp.float32
BF16 = jnp.bfloat16
MESH = pl.DeviceIdType.MESH
NEAR = tuple((dr, dq) for dr in (-1, 0, 1) for dq in (-1, 0, 1) if (dr, dq) != (0, 0))
WIDE = tuple((dr, dq) for dr in (-2, -1, 0, 1, 2) for dq in (-1, 0, 1))
HB = 32
WB = 256
WE = 384
OWN = 9


def dot(a, b):
    return lax.dot_general(a, b, (((1,), (0,)), ((), ())), preferred_element_type=F32)


def dot_t(a, b):
    return lax.dot_general(a, b, (((1,), (1,)), ((), ())), preferred_element_type=F32)


def split2(x):
    high = x.astype(BF16)
    return high, (x - high.astype(F32)).astype(BF16)


def split3(x):
    high = x.astype(BF16)
    rest = x - high.astype(F32)
    middle = rest.astype(BF16)
    return high, middle, (rest - middle.astype(F32)).astype(BF16)


def kernel(
    n_rows,
    n_cols,
    n_ty,
    noisy_h, w_in_h, kf_h, wd_h, kc_h, wu_h, kl_h, wo_h, cell_h, count_h, obs_h,
    out_h,
    noisy_v, w_in_v, kf_v, wd_v, kc_v, wu_v, kl_v, wo_v, cell_v, count_v, obs_v,
    row_send, col_send, row_recv, col_recv, pool_send, pool_recv,
    ext, taps, taps_h, taps_l, a1, a2, w9, wo8, expand, fine, fine_l, fine_r, acc,
    station_a, station_b, fine_three, coarse, up_b, s_ref, raised_ref, out_v,
    in_sem, out_sem, near_send, near_recv, wide_send, wide_recv,
):
    row = lax.axis_index("grp") * n_ty + lax.axis_index("ty")
    col = lax.axis_index("tx")

    def device(dr, dq):
        r = lax.rem(row + dr + n_rows, n_rows)
        q = lax.rem(col + dq + n_cols, n_cols)
        return (r // n_ty, lax.rem(r, n_ty), q)

    def row_ok(dr):
        return jnp.logical_and(row + dr >= 0, row + dr < n_rows)

    def col_ok(dq):
        return jnp.logical_and(col + dq >= 0, col + dq < n_cols)

    pairs = (
        (noisy_h, noisy_v), (w_in_h, w_in_v), (kf_h, kf_v), (kl_h, kl_v), (wo_h, wo_v), (cell_h, cell_v),
        (count_h, count_v), (obs_h, obs_v), (wd_h, wd_v), (wu_h, wu_v), (kc_h, kc_v),
    )
    loads = [pltpu.make_async_copy(src, dst, in_sem.at[k]) for k, (src, dst) in enumerate(pairs)]
    for load in loads:
        load.start()

    barrier = pltpu.get_barrier_semaphore()
    for dr, dq in WIDE:
        if (dr, dq) != (0, 0):
            pl.semaphore_signal(barrier, inc=1, device_id=device(dr, dq), device_id_type=MESH)

    loads[0].wait()
    for v in range(4):
        row_send[0, 2 * v : 2 * v + 2, :] = noisy_v[v, 0:2, :]
        row_send[1, 2 * v : 2 * v + 2, :] = noisy_v[v, HB - 2 : HB, :]
    first = jnp.concatenate([noisy_v[v, :, 0:128] for v in range(4)], axis=0)
    last = jnp.concatenate([noisy_v[v, :, 128:256] for v in range(4)], axis=0)
    col_send[0] = first.T[0:8, :]
    col_send[1] = last.T[120:128, :]

    pl.semaphore_wait(barrier, len(WIDE) - 1)
    near = []
    for k, (dr, dq) in enumerate(NEAR):
        if dq == 0:
            src = row_send.at[0 if dr < 0 else 1]
            dst = row_recv.at[1 if dr < 0 else 0]
        else:
            src = col_send.at[0 if dq < 0 else 1]
            dst = col_recv.at[1 if dq < 0 else 0, 1 - dr]
        back = NEAR.index((-dr, -dq))
        near.append(
            pltpu.make_async_remote_copy(
                src_ref=src, dst_ref=dst, send_sem=near_send.at[k], recv_sem=near_recv.at[back],
                device_id=device(dr, dq), device_id_type=MESH,
            )
        )
    for copy in near:
        copy.start()

    for load in loads[1:]:
        load.wait()
    w_tiled = dot_hi(w_in_v[...].T)
    lane = lax.broadcasted_iota(jnp.int32, (64, 128), 1)
    zero64 = jnp.zeros((64, 64), BF16)
    kf9 = jnp.concatenate([kf_v[p, q] for p in range(3) for q in range(3)], axis=1)
    for r in range(4):
        placed = []
        for p in range(3):
            for q in range(3):
                at = 12 * (r + p) + 4 * q
                placed.append(jnp.where(jnp.logical_and(lane >= at, lane < at + 4), w_tiled, 0.0))
        placed = jnp.concatenate(placed, axis=0)
        high, middle, low = split3(placed)
        conv = 0.5 * (dot(kf9, high) + dot(kf9, middle) + dot(kf9, low))
        at = 12 * (r + 1) + 4
        lift = jnp.where(jnp.logical_and(lane >= at, lane < at + 4), w_tiled, 0.0)
        high, low = split2(jnp.concatenate([conv, lift], axis=0))
        a1[r, :, 0:80] = high[:, 0:80]
        a1[r, :, 80:160] = high[:, 0:80]
        a1[r, :, 160:240] = low[:, 0:80]
    half = [[(kl_v[p, q].astype(F32) * 0.5).astype(BF16) for q in range(3)] for p in range(3)]
    for q in range(3):
        upper = jnp.concatenate([half[0][q], half[1][q], half[2][q], zero64], axis=1)
        lower = jnp.concatenate([zero64, half[0][q], half[1][q], half[2][q]], axis=1)
        a2[q] = jnp.concatenate([upper, lower], axis=0)
    w9[...] = jnp.concatenate([half[p][q] for p in range(3) for q in range(3)], axis=1)
    pick = (lax.broadcasted_iota(jnp.int32, (32, 4), 0) // 8 == lax.broadcasted_iota(jnp.int32, (32, 4), 1))
    spread = dot(pick.astype(BF16), wo_v[...])
    spread = jnp.concatenate([spread] * 8, axis=1)
    same = lax.broadcasted_iota(jnp.int32, (32, 512), 0) % 8 == lax.broadcasted_iota(jnp.int32, (32, 512), 1) // 64
    wo8[...] = jnp.where(same, spread, 0.0).astype(BF16)
    cells = lax.broadcasted_iota(jnp.int32, (72, WB), 0)
    pixel = lax.broadcasted_iota(jnp.int32, (72, WB), 1)
    for rho in range(3):
        for q in range(3):
            want = rho * 24 + 7 + (pixel + (32 + q - 1)) // 32
            expand[rho * 3 + q] = (cells == want).astype(F32).astype(BF16)

    cell = cell_v[0]
    count = count_v[0].astype(F32)
    at_row = (lax.broadcasted_iota(jnp.int32, (HB, 128), 0) == cell // WB).astype(F32)
    at_col = (lax.broadcasted_iota(jnp.int32, (WB, 128), 0) == cell % WB).astype(F32).astype(BF16)
    reports = [at_row * (count * obs_v[v, 0]) for v in range(4)] + [at_row * count]
    parts = split3(jnp.concatenate(reports, axis=0))
    sums = dot_t(parts[0], at_col) + dot_t(parts[1], at_col) + dot_t(parts[2], at_col)
    for v in range(4):
        station_a[v] = 0.5 * noisy_v[v] + 0.25 * sums[HB * v : HB * (v + 1)]
    station_b[...] = 0.5 - 0.25 * sums[HB * 4 :]

    for k, (dr, dq) in enumerate(NEAR):
        if dr >= 0:
            near[k].wait_recv()
    ext[...] = jnp.zeros_like(ext)

    def side_columns(k):
        right = jnp.where(jnp.logical_and(row_ok(k - 1), col_ok(1)), col_recv[1, k], 0.0)
        left = jnp.where(jnp.logical_and(row_ok(k - 1), col_ok(-1)), col_recv[0, k], 0.0)
        return jnp.concatenate([right, jnp.zeros((112, 128), F32), left], axis=0).T

    above, beside = side_columns(0), side_columns(1)
    for v in range(4):
        ext[v, OWN : OWN + HB, 0:WB] = noisy_v[v]
        ext[v, OWN - 2 : OWN, 0:WB] = jnp.where(row_ok(-1), row_recv[0, 2 * v : 2 * v + 2, :], 0.0)
        ext[v, OWN - 2 : OWN, WB:WE] = above[HB * v + HB - 2 : HB * v + HB]
        ext[v, OWN : OWN + HB, WB:WE] = beside[HB * v : HB * (v + 1)]

    def make_taps(start, size):
        for v in range(4):
            for t in range(3):
                here, before, after = (
                    ext[v, start : start + size, 128 * ((t + d) % 3) : 128 * ((t + d) % 3) + 128] for d in (0, 2, 1)
                )
                spot = lax.broadcasted_iota(jnp.int32, here.shape, 1)
                shifted = (
                    jnp.where(spot < 1, pltpu.roll(before, 1, 1), pltpu.roll(here, 1, 1)),
                    here,
                    jnp.where(spot < 127, pltpu.roll(here, 127, 1), pltpu.roll(after, 127, 1)),
                )
                for q in range(3):
                    taps[t, pl.ds(12 * start + 4 * q + v, size, stride=12), :] = shifted[q]
        rows = slice(12 * start, 12 * (start + size))
        for t in range(3):
            high, low = split2(taps[t, rows])
            taps_h[rows, 128 * t : 128 * t + 128] = high
            taps_l[rows, 128 * t : 128 * t + 128] = low

    make_taps(0, 48)

    def window(at, lanes):
        high = taps_h[pl.ds(at, 80), lanes]
        return jnp.concatenate([high, taps_l[pl.ds(at, 80), lanes], high], axis=0)

    def gated(both):
        h = both[0:64]
        return both[64:128] + (h + h * jnp.tanh(h))

    def fine_row(i, rhs, gate=None):
        value = gated(dot(a1[i % 4], rhs))
        if gate is not None:
            value = value * jnp.where(gate, 1.0, 0.0)
        fine[64 * (i + 1) : 64 * (i + 2), 0:WB] = value.astype(BF16)
        return value

    into = lax.broadcasted_iota(jnp.int32, (8, WB), 1) // 32 == lax.broadcasted_iota(jnp.int32, (8, WB), 0)
    into = into.astype(F32).astype(BF16)

    def sums_of(upper, lower):
        high, low = split2(jnp.concatenate([upper, lower], axis=0))
        return (dot_t(into, high) + dot_t(into, low)) * (1.0 / 1024.0)

    middle = jnp.zeros((64, WB), F32)
    for g in range(8):
        rhs = window(96 + 48 * g, slice(0, WB))
        for r in range(4):
            i = 4 * g + r
            if i < HB - 1:
                value = fine_row(i, rhs)
                if i == 0:
                    first_row = value
                else:
                    middle = middle + value
    outer_row = fine_row(-1, window(48, slice(0, WB)), row_ok(-1))
    tile = sums_of(middle + first_row, outer_row)
    pool_send[0] = tile
    wide = []

    def send(which, dr, dq, slot):
        wide.append(
            pltpu.make_async_remote_copy(
                src_ref=pool_send.at[which], dst_ref=pool_recv.at[slot], send_sem=wide_send.at[len(wide)],
                recv_sem=wide_recv.at[slot], device_id=device(dr, dq), device_id_type=MESH,
            )
        )
        wide[-1].start()

    for dr in (1, 2):
        for dq in (-1, 0, 1):
            send(0, dr, dq, WIDE.index((-dr, -dq)))
    for dq in (-1, 1):
        send(0, 0, dq, WIDE.index((0, -dq)))
    pool_recv[WIDE.index((0, 0))] = tile

    for k, (dr, dq) in enumerate(NEAR):
        if dr < 0:
            near[k].wait_recv()
    below = side_columns(2)
    for v in range(4):
        ext[v, OWN + HB : OWN + HB + 2, 0:WB] = jnp.where(row_ok(1), row_recv[1, 2 * v : 2 * v + 2, :], 0.0)
        ext[v, OWN + HB : OWN + HB + 2, WB:WE] = below[HB * v : HB * v + 2]
    make_taps(40, 8)
    last_row = fine_row(HB - 1, window(432, slice(0, WB)))
    outer_row = fine_row(HB, window(480, slice(0, WB)), row_ok(1))
    pool_send[1] = sums_of(middle + last_row, outer_row)
    tile = sums_of(middle + first_row + last_row, outer_row)
    pool_send[2] = tile
    for dr in (-1, -2):
        for dq in (-1, 0, 1):
            send(1, dr, dq, WIDE.index((-dr, -dq)))
    for dq in (-1, 1):
        send(2, 0, dq, 16 - dq)
    pool_recv[16] = tile

    side_lane = lax.broadcasted_iota(jnp.int32, (64, 128), 1)
    right_gate = jnp.where(col_ok(1), 1.0, 0.0)
    left_gate = jnp.where(col_ok(-1), 1.0, 0.0)
    side_gate = jnp.where(side_lane < 64, right_gate, left_gate)

    def side_rows(g, carry):
        rhs = jnp.concatenate(
            [
                window(pl.multiple_of(96 + 96 * g, 16), slice(WB, WE)),
                window(pl.multiple_of(144 + 96 * g, 16), slice(WB, WE)),
            ],
            axis=1,
        )
        for r in range(4):
            value = gated(dot(a1[r], rhs))
            for k in range(2):
                at = pl.multiple_of((8 * g + 4 * k + r + 1) * 64, 64)
                fine[pl.ds(at, 64), WB:WE] = (value[:, 128 * k : 128 * k + 128] * side_gate).astype(BF16)
        return carry

    lax.fori_loop(0, 4, side_rows, 0, unroll=True)
    for at, r, e, gate in ((48, 3, 0, row_ok(-1)), (480, 0, 33, row_ok(1))):
        gate = jnp.where(gate, 1.0, 0.0)
        value = gated(dot(a1[r], window(at, slice(WB, WE)))) * side_gate * gate
        fine[e * 64 : e * 64 + 64, WB:WE] = value.astype(BF16)

    def shift_rows(e, carry):
        at = pl.multiple_of(e * 64, 64)
        tile = [fine[pl.ds(at, 64), 128 * t : 128 * t + 128] for t in range(3)]
        spot = lax.broadcasted_iota(jnp.int32, (64, 128), 1)
        tile = [x.astype(F32) for x in tile]
        up = [pltpu.roll(x, 1, 1) for x in tile]
        down = [pltpu.roll(x, 127, 1) for x in tile]
        fine_l[pl.ds(at, 64), 0:128] = jnp.where(spot < 1, up[2], up[0]).astype(BF16)
        fine_l[pl.ds(at, 64), 128:256] = jnp.where(spot < 1, up[0], up[1]).astype(BF16)
        fine_r[pl.ds(at, 64), 0:128] = jnp.where(spot < 127, down[0], down[1]).astype(BF16)
        fine_r[pl.ds(at, 64), 128:256] = jnp.where(spot < 127, down[1], down[2]).astype(BF16)
        return carry

    lax.fori_loop(0, HB + 2, shift_rows, 0, unroll=True)

    def last_rows(k, carry):
        at = pl.multiple_of(k * 128, 128)
        total = dot(a2[0], fine_l[pl.ds(at, 256), :])
        total += dot(a2[1], fine[pl.ds(at, 256), 0:WB])
        total += dot(a2[2], fine_r[pl.ds(at, 256), :])
        acc[pl.ds(at, 128), :] = total
        return carry

    lax.fori_loop(0, 16, last_rows, 0, unroll=True)

    for copy in wide:
        copy.wait()
    for copy in near:
        copy.wait_send()
    cells = []
    for dr, dq in WIDE:
        if dr == 0:
            cell = pool_recv[16 + dq]
        else:
            step = 1 if dr > 0 else -1
            if dr == 1:
                other = pool_recv[16 + dq]
            else:
                other = pool_recv[WIDE.index((dr - step, dq))]
            cell = pool_recv[WIDE.index((dr, dq))] + pltpu.roll(other, 64, 1)
        cells.append(jnp.where(jnp.logical_and(row_ok(dr), col_ok(dq)), cell, 0.0))
    cells = jnp.concatenate(cells, axis=0).astype(BF16)
    entering = dot(cells[:, 0:64], wd_v[...])
    coarse[0:8] = jnp.zeros((8, 256), F32)
    coarse[128:136] = jnp.zeros((8, 256), F32)
    coarse[8:128] = entering.astype(BF16).astype(F32)
    total = jnp.zeros((72, 256), F32)
    for p in range(3):
        for q in range(3):
            at = 8 + 24 * p + q - 1
            total += dot_t(coarse[at : at + 72].astype(BF16), kc_v[p, q])
    half_total = 0.5 * total
    leaving = coarse[32:104] + (half_total + half_total * jnp.tanh(half_total))
    blocks = []
    for k, (dr, dq) in enumerate(WIDE[3:12]):
        block = leaving[8 * k : 8 * k + 8]
        blocks.append(jnp.where(jnp.logical_and(row_ok(dr), col_ok(dq)), block, 0.0))
    leaving = jnp.concatenate(blocks, axis=0).astype(BF16)
    high, low = split2(dot_t(wu_v[...], leaving))
    for k in range(9):
        wide_up = dot(high, expand[k])
        up_b[k] = wide_up.astype(BF16)
        if k == 4:
            raised_ref[...] = wide_up + dot(low, expand[k])
    for edge, rhos in enumerate(((0, 1, 1), (1, 1, 1), (1, 1, 2))):
        rhs = jnp.concatenate([up_b[rhos[p] * 3 + q] for p in range(3) for q in range(3)], axis=0)
        s_ref[edge] = dot(w9[...], rhs)

    def finish(i, edge):
        at = i * 64 if isinstance(i, int) else pl.multiple_of(i * 64, 64)
        h = acc[pl.ds(at, 64), :] + s_ref[edge]
        one = fine[pl.ds(at + 64, 64), 0:WB].astype(F32)
        value = one + raised_ref[...] + (h + h * jnp.tanh(h))
        fine_three[pl.ds(at, 64), :] = value.astype(BF16)

    def finish_middle(i, carry):
        finish(i, 1)
        return carry

    finish(0, 0)
    finish(HB - 1, 2)
    lax.fori_loop(1, HB - 1, finish_middle, 0, unroll=True)
    for g in range(4):
        denoised = dot(wo8[...], fine_three[512 * g : 512 * g + 512, :])
        for v in range(4):
            rows = slice(8 * g, 8 * g + 8)
            out_v[v, rows, :] = station_a[v, rows, :] + station_b[rows, :] * denoised[8 * v : 8 * v + 8]
    store = pltpu.make_async_copy(out_v, out_h, out_sem)
    store.start()
    store.wait()


def dot_hi(w_in):
    place = lax.broadcasted_iota(jnp.int32, (4, 128), 1) % 4 == lax.broadcasted_iota(jnp.int32, (4, 128), 0)
    place = place.astype(F32).astype(BF16)
    high, middle, low = split3(w_in)
    return (dot(high, place) + dot(middle, place)) + dot(low, place)


def solution(mesh):
    n_ty = mesh.shape["ty"]
    n_rows = mesh.shape["grp"] * n_ty
    n_cols = mesh.shape["tx"]

    def on_device(noisy, w_in, kf, wd, kc, wu, kl, wo, cell, count, obs):
        w_in, wd = w_in.T, wd.T
        obs = obs.reshape(4, 1, 128)
        cell = cell.reshape(1, 1, 128)
        count = count.reshape(1, 1, 128)
        args = (noisy, w_in, kf, wd, kc, wu, kl, wo, cell, count, obs)
        vmem = pltpu.VMEM
        return pl.pallas_call(
            functools.partial(kernel, n_rows, n_cols, n_ty),
            out_shape=jax.ShapeDtypeStruct(noisy.shape, noisy.dtype),
            in_specs=[pl.BlockSpec(memory_space=pltpu.HBM)] * 11,
            out_specs=pl.BlockSpec(memory_space=pl.ANY),
            scratch_shapes=[vmem(x.shape, x.dtype) for x in args]
            + [
                vmem((2, 8, WB), F32),
                vmem((2, 8, 128), F32),
                vmem((2, 8, WB), F32),
                vmem((2, 3, 8, 128), F32),
                vmem((3, 8, 128), F32),
                vmem((18, 8, 128), F32),
                vmem((4, 48, WE), F32),
                vmem((3, 576, 128), F32),
                vmem((576, WE), BF16),
                vmem((576, WE), BF16),
                vmem((4, 128, 240), BF16),
                vmem((3, 128, 256), BF16),
                vmem((64, 576), BF16),
                vmem((32, 512), BF16),
                vmem((9, 72, WB), BF16),
                vmem((34 * 64, WE), BF16),
                vmem((34 * 64, WB), BF16),
                vmem((34 * 64, WB), BF16),
                vmem((HB * 64, WB), F32),
                vmem((4, HB, WB), F32),
                vmem((HB, WB), F32),
                vmem((HB * 64, WB), BF16),
                vmem((136, 256), F32),
                vmem((9, 64, WB), BF16),
                vmem((3, 64, WB), F32),
                vmem((64, WB), F32),
                vmem((4, HB, WB), F32),
                pltpu.SemaphoreType.DMA((11,)),
                pltpu.SemaphoreType.DMA,
                pltpu.SemaphoreType.DMA((8,)),
                pltpu.SemaphoreType.DMA((8,)),
                pltpu.SemaphoreType.DMA((16,)),
                pltpu.SemaphoreType.DMA((18,)),
            ],
            compiler_params=pltpu.CompilerParams(
                collective_id=0, has_side_effects=True, vmem_limit_bytes=67043328
            ),
        )(*args)

    return jax.shard_map(
        on_device,
        mesh=mesh,
        in_specs=(
            P(None, ("grp", "ty"), "tx"),
            P(),
            P(),
            P(),
            P(),
            P(),
            P(),
            P(),
            P(("grp", "ty"), "tx", None),
            P(("grp", "ty"), "tx", None),
            P(None, ("grp", "ty"), "tx", None),
        ),
        out_specs=P(None, ("grp", "ty"), "tx"),
        check_vma=False,
    )
```

```python
import functools

import jax
import jax.numpy as jnp
from jax import lax
from jax.experimental import pallas as pl
from jax.experimental.pallas import tpu as pltpu
from jax.sharding import PartitionSpec as P

F32 = jnp.float32
BF16 = jnp.bfloat16
MESH = pl.DeviceIdType.MESH
NEAR = tuple((dr, dq) for dr in (-1, 0, 1) for dq in (-1, 0, 1) if (dr, dq) != (0, 0))
WIDE = tuple((dr, dq) for dr in (-2, -1, 0, 1, 2) for dq in (-1, 0, 1))
HB = 32
WB = 256
WE = 384
OWN = 9


def dot(a, b):
    return lax.dot_general(a, b, (((1,), (0,)), ((), ())), preferred_element_type=F32)


def dot_t(a, b):
    return lax.dot_general(a, b, (((1,), (1,)), ((), ())), preferred_element_type=F32)


def split2(x):
    high = x.astype(BF16)
    return high, (x - high.astype(F32)).astype(BF16)


def split3(x):
    high = x.astype(BF16)
    rest = x - high.astype(F32)
    middle = rest.astype(BF16)
    return high, middle, (rest - middle.astype(F32)).astype(BF16)


def kernel(
    n_rows,
    n_cols,
    n_ty,
    noisy_h, w_in_h, kf_h, wd_h, kc_h, wu_h, kl_h, wo_h, cell_h, count_h, obs_h,
    out_h,
    noisy_v, w_in_v, kf_v, wd_v, kc_v, wu_v, kl_v, wo_v, cell_v, count_v, obs_v,
    row_send, col_send, row_recv, col_recv, pool_send, pool_recv,
    ext, taps, taps_h, taps_l, a1, a2, w9, wo8, expand, fine, fine_l, fine_r, acc,
    station_a, station_b, fine_three, coarse, up_b, s_ref, raised_ref,
    in_sem, near_send, near_recv, wide_send, wide_recv,
):
    row = lax.axis_index("grp") * n_ty + lax.axis_index("ty")
    col = lax.axis_index("tx")

    def device(dr, dq):
        r = lax.rem(row + dr + n_rows, n_rows)
        q = lax.rem(col + dq + n_cols, n_cols)
        return (r // n_ty, lax.rem(r, n_ty), q)

    def row_ok(dr):
        return jnp.logical_and(row + dr >= 0, row + dr < n_rows)

    def col_ok(dq):
        return jnp.logical_and(col + dq >= 0, col + dq < n_cols)

    pairs = (
        (noisy_h, noisy_v), (w_in_h, w_in_v), (kf_h, kf_v), (kl_h, kl_v), (wo_h, wo_v), (cell_h, cell_v),
        (count_h, count_v), (obs_h, obs_v), (wd_h, wd_v), (wu_h, wu_v), (kc_h, kc_v),
    )
    loads = [pltpu.make_async_copy(src, dst, in_sem.at[k]) for k, (src, dst) in enumerate(pairs)]
    for load in loads:
        load.start()

    def there(dr, dq):
        if dq == 0:
            return row_ok(dr)
        return col_ok(dq) if dr == 0 else jnp.logical_and(row_ok(dr), col_ok(dq))

    barrier = pltpu.get_barrier_semaphore()
    for dr, dq in WIDE:
        if (dr, dq) != (0, 0):

            @pl.when(there(dr, dq))
            def _(dr=dr, dq=dq):
                pl.semaphore_signal(barrier, inc=1, device_id=device(dr, dq), device_id_type=MESH)


    loads[0].wait()
    for v in range(4):
        row_send[0, 2 * v : 2 * v + 2, :] = noisy_v[v, 0:2, :]
        row_send[1, 2 * v : 2 * v + 2, :] = noisy_v[v, HB - 2 : HB, :]
    first = jnp.concatenate([noisy_v[v, :, 0:128] for v in range(4)], axis=0)
    last = jnp.concatenate([noisy_v[v, :, 128:256] for v in range(4)], axis=0)
    col_send[0] = first.T[0:8, :]
    col_send[1] = last.T[120:128, :]

    above_count = jnp.minimum(row, 2)
    below_count = jnp.minimum(n_rows - 1 - row, 2)
    sides = jnp.minimum(col, 1) + jnp.minimum(n_cols - 1 - col, 1)
    pl.semaphore_wait(barrier, (above_count + below_count + 1) * (sides + 1) - 1)
    near = []
    for k, (dr, dq) in enumerate(NEAR):
        if dq == 0:
            src = row_send.at[0 if dr < 0 else 1]
            dst = row_recv.at[1 if dr < 0 else 0]
        else:
            src = col_send.at[0 if dq < 0 else 1]
            dst = col_recv.at[1 if dq < 0 else 0, 1 - dr]
        back = NEAR.index((-dr, -dq))
        near.append(
            pltpu.make_async_remote_copy(
                src_ref=src, dst_ref=dst, send_sem=near_send.at[k], recv_sem=near_recv.at[back],
                device_id=device(dr, dq), device_id_type=MESH,
            )
        )
    for copy, (dr, dq) in zip(near, NEAR):
        pl.when(there(dr, dq))(copy.start)

    for load in loads[1:]:
        load.wait()
    w_tiled = dot_hi(w_in_v[...].T)
    lane = lax.broadcasted_iota(jnp.int32, (64, 128), 1)
    zero64 = jnp.zeros((64, 64), BF16)
    kf9 = jnp.concatenate([kf_v[p, q] for p in range(3) for q in range(3)], axis=1)
    for r in range(4):
        placed = []
        for p in range(3):
            for q in range(3):
                at = 12 * (r + p) + 4 * q
                placed.append(jnp.where(jnp.logical_and(lane >= at, lane < at + 4), w_tiled, 0.0))
        placed = jnp.concatenate(placed, axis=0)
        high, middle, low = split3(placed)
        conv = 0.5 * (dot(kf9, high) + dot(kf9, middle) + dot(kf9, low))
        at = 12 * (r + 1) + 4
        lift = jnp.where(jnp.logical_and(lane >= at, lane < at + 4), w_tiled, 0.0)
        high, low = split2(jnp.concatenate([conv, lift], axis=0))
        a1[r, :, 0:80] = high[:, 0:80]
        a1[r, :, 80:160] = high[:, 0:80]
        a1[r, :, 160:240] = low[:, 0:80]
    half = [[(kl_v[p, q].astype(F32) * 0.5).astype(BF16) for q in range(3)] for p in range(3)]
    for q in range(3):
        upper = jnp.concatenate([half[0][q], half[1][q], half[2][q], zero64], axis=1)
        lower = jnp.concatenate([zero64, half[0][q], half[1][q], half[2][q]], axis=1)
        a2[q] = jnp.concatenate([upper, lower], axis=0)
    w9[...] = jnp.concatenate([half[p][q] for p in range(3) for q in range(3)], axis=1)
    pick = (lax.broadcasted_iota(jnp.int32, (32, 4), 0) // 8 == lax.broadcasted_iota(jnp.int32, (32, 4), 1))
    spread = dot(pick.astype(BF16), wo_v[...])
    spread = jnp.concatenate([spread] * 8, axis=1)
    same = lax.broadcasted_iota(jnp.int32, (32, 512), 0) % 8 == lax.broadcasted_iota(jnp.int32, (32, 512), 1) // 64
    wo8[...] = jnp.where(same, spread, 0.0).astype(BF16)
    cells = lax.broadcasted_iota(jnp.int32, (72, WB), 0)
    pixel = lax.broadcasted_iota(jnp.int32, (72, WB), 1)
    for rho in range(3):
        for q in range(3):
            want = rho * 24 + 7 + (pixel + (32 + q - 1)) // 32
            expand[rho * 3 + q] = (cells == want).astype(F32).astype(BF16)

    cell = cell_v[0]
    count = count_v[0].astype(F32)
    at_row = (lax.broadcasted_iota(jnp.int32, (HB, 128), 0) == cell // WB).astype(F32)
    at_col = (lax.broadcasted_iota(jnp.int32, (WB, 128), 0) == cell % WB).astype(F32).astype(BF16)
    reports = [at_row * (count * obs_v[v, 0]) for v in range(4)] + [at_row * count]
    parts = split3(jnp.concatenate(reports, axis=0))
    sums = dot_t(parts[0], at_col) + dot_t(parts[1], at_col) + dot_t(parts[2], at_col)
    for v in range(4):
        station_a[v] = 0.5 * noisy_v[v] + 0.25 * sums[HB * v : HB * (v + 1)]
    station_b[...] = 0.5 - 0.25 * sums[HB * 4 :]

    for k, (dr, dq) in enumerate(NEAR):
        if dr >= 0:
            pl.when(there(-dr, -dq))(near[k].wait_recv)
    ext[...] = jnp.zeros_like(ext)

    def side_columns(k):
        right = jnp.where(jnp.logical_and(row_ok(k - 1), col_ok(1)), col_recv[1, k], 0.0)
        left = jnp.where(jnp.logical_and(row_ok(k - 1), col_ok(-1)), col_recv[0, k], 0.0)
        return jnp.concatenate([right, jnp.zeros((112, 128), F32), left], axis=0).T

    above, beside = side_columns(0), side_columns(1)
    for v in range(4):
        ext[v, OWN : OWN + HB, 0:WB] = noisy_v[v]
        ext[v, OWN - 2 : OWN, 0:WB] = jnp.where(row_ok(-1), row_recv[0, 2 * v : 2 * v + 2, :], 0.0)
        ext[v, OWN - 2 : OWN, WB:WE] = above[HB * v + HB - 2 : HB * v + HB]
        ext[v, OWN : OWN + HB, WB:WE] = beside[HB * v : HB * (v + 1)]

    def make_taps(start, size):
        for v in range(4):
            for t in range(3):
                here, before, after = (
                    ext[v, start : start + size, 128 * ((t + d) % 3) : 128 * ((t + d) % 3) + 128] for d in (0, 2, 1)
                )
                spot = lax.broadcasted_iota(jnp.int32, here.shape, 1)
                shifted = (
                    jnp.where(spot < 1, pltpu.roll(before, 1, 1), pltpu.roll(here, 1, 1)),
                    here,
                    jnp.where(spot < 127, pltpu.roll(here, 127, 1), pltpu.roll(after, 127, 1)),
                )
                for q in range(3):
                    taps[t, pl.ds(12 * start + 4 * q + v, size, stride=12), :] = shifted[q]
        rows = slice(12 * start, 12 * (start + size))
        for t in range(3):
            high, low = split2(taps[t, rows])
            taps_h[rows, 128 * t : 128 * t + 128] = high
            taps_l[rows, 128 * t : 128 * t + 128] = low

    make_taps(0, 48)

    def window(at, lanes):
        high = taps_h[pl.ds(at, 80), lanes]
        return jnp.concatenate([high, taps_l[pl.ds(at, 80), lanes], high], axis=0)

    def gated(both):
        h = both[0:64]
        return both[64:128] + (h + h * jnp.tanh(h))

    def fine_row(i, rhs, gate=None):
        value = gated(dot(a1[i % 4], rhs))
        if gate is not None:
            value = value * jnp.where(gate, 1.0, 0.0)
        fine[64 * (i + 1) : 64 * (i + 2), 0:WB] = value.astype(BF16)
        return value

    into = lax.broadcasted_iota(jnp.int32, (8, WB), 1) // 32 == lax.broadcasted_iota(jnp.int32, (8, WB), 0)
    into = into.astype(F32).astype(BF16)

    def sums_of(upper, lower):
        high, low = split2(jnp.concatenate([upper, lower], axis=0))
        return (dot_t(into, high) + dot_t(into, low)) * (1.0 / 1024.0)

    middle = jnp.zeros((64, WB), F32)
    for g in range(8):
        rhs = window(96 + 48 * g, slice(0, WB))
        for r in range(4):
            i = 4 * g + r
            if i < HB - 1:
                value = fine_row(i, rhs)
                if i == 0:
                    first_row = value
                else:
                    middle = middle + value
    outer_row = fine_row(-1, window(48, slice(0, WB)), row_ok(-1))
    tile = sums_of(middle + first_row, outer_row)
    pool_send[0] = tile
    wide, wide_at = [], []

    def send(which, dr, dq, slot):
        wide.append(
            pltpu.make_async_remote_copy(
                src_ref=pool_send.at[which], dst_ref=pool_recv.at[slot], send_sem=wide_send.at[len(wide)],
                recv_sem=wide_recv.at[slot], device_id=device(dr, dq), device_id_type=MESH,
            )
        )
        pl.when(there(dr, dq))(wide[-1].start)
        wide_at.append((dr, dq))

    for dr in (1, 2):
        for dq in (-1, 0, 1):
            send(0, dr, dq, WIDE.index((-dr, -dq)))
    for dq in (-1, 1):
        send(0, 0, dq, WIDE.index((0, -dq)))
    pool_recv[WIDE.index((0, 0))] = tile

    for k, (dr, dq) in enumerate(NEAR):
        if dr < 0:
            pl.when(there(-dr, -dq))(near[k].wait_recv)
    below = side_columns(2)
    for v in range(4):
        ext[v, OWN + HB : OWN + HB + 2, 0:WB] = jnp.where(row_ok(1), row_recv[1, 2 * v : 2 * v + 2, :], 0.0)
        ext[v, OWN + HB : OWN + HB + 2, WB:WE] = below[HB * v : HB * v + 2]
    make_taps(40, 8)
    last_row = fine_row(HB - 1, window(432, slice(0, WB)))
    outer_row = fine_row(HB, window(480, slice(0, WB)), row_ok(1))
    pool_send[1] = sums_of(middle + last_row, outer_row)
    tile = sums_of(middle + first_row + last_row, outer_row)
    pool_send[2] = tile
    for dr in (-1, -2):
        for dq in (-1, 0, 1):
            send(1, dr, dq, WIDE.index((-dr, -dq)))
    for dq in (-1, 1):
        send(2, 0, dq, 16 - dq)
    pool_recv[16] = tile

    side_lane = lax.broadcasted_iota(jnp.int32, (64, 128), 1)
    right_gate = jnp.where(col_ok(1), 1.0, 0.0)
    left_gate = jnp.where(col_ok(-1), 1.0, 0.0)
    side_gate = jnp.where(side_lane < 64, right_gate, left_gate)

    def side_rows(g, carry):
        rhs = jnp.concatenate(
            [
                window(pl.multiple_of(96 + 96 * g, 16), slice(WB, WE)),
                window(pl.multiple_of(144 + 96 * g, 16), slice(WB, WE)),
            ],
            axis=1,
        )
        for r in range(4):
            value = gated(dot(a1[r], rhs))
            for k in range(2):
                at = pl.multiple_of((8 * g + 4 * k + r + 1) * 64, 64)
                fine[pl.ds(at, 64), WB:WE] = (value[:, 128 * k : 128 * k + 128] * side_gate).astype(BF16)
        return carry

    lax.fori_loop(0, 4, side_rows, 0, unroll=True)
    for at, r, e, gate in ((48, 3, 0, row_ok(-1)), (480, 0, 33, row_ok(1))):
        gate = jnp.where(gate, 1.0, 0.0)
        value = gated(dot(a1[r], window(at, slice(WB, WE)))) * side_gate * gate
        fine[e * 64 : e * 64 + 64, WB:WE] = value.astype(BF16)

    def shift_rows(e, carry):
        at = pl.multiple_of(e * 64, 64)
        tile = [fine[pl.ds(at, 64), 128 * t : 128 * t + 128] for t in range(3)]
        spot = lax.broadcasted_iota(jnp.int32, (64, 128), 1)
        tile = [x.astype(F32) for x in tile]
        up = [pltpu.roll(x, 1, 1) for x in tile]
        down = [pltpu.roll(x, 127, 1) for x in tile]
        fine_l[pl.ds(at, 64), 0:128] = jnp.where(spot < 1, up[2], up[0]).astype(BF16)
        fine_l[pl.ds(at, 64), 128:256] = jnp.where(spot < 1, up[0], up[1]).astype(BF16)
        fine_r[pl.ds(at, 64), 0:128] = jnp.where(spot < 127, down[0], down[1]).astype(BF16)
        fine_r[pl.ds(at, 64), 128:256] = jnp.where(spot < 127, down[1], down[2]).astype(BF16)
        return carry

    lax.fori_loop(0, HB + 2, shift_rows, 0, unroll=True)

    def last_rows(k, carry):
        at = pl.multiple_of(k * 128, 128)
        total = dot(a2[0], fine_l[pl.ds(at, 256), :])
        total += dot(a2[1], fine[pl.ds(at, 256), 0:WB])
        total += dot(a2[2], fine_r[pl.ds(at, 256), :])
        acc[pl.ds(at, 128), :] = total
        return carry

    lax.fori_loop(0, 16, last_rows, 0, unroll=True)

    for copy, (dr, dq) in zip(wide, wide_at):
        pl.when(there(-dr, -dq))(copy.wait_recv)
    for copy, (dr, dq) in zip(wide + near, wide_at + list(NEAR)):
        pl.when(there(dr, dq))(copy.wait_send)
    cells = []
    for dr, dq in WIDE:
        if dr == 0:
            cell = pool_recv[16 + dq]
        else:
            step = 1 if dr > 0 else -1
            if dr == 1:
                other = pool_recv[16 + dq]
            else:
                other = pool_recv[WIDE.index((dr - step, dq))]
            cell = pool_recv[WIDE.index((dr, dq))] + pltpu.roll(other, 64, 1)
        cells.append(jnp.where(jnp.logical_and(row_ok(dr), col_ok(dq)), cell, 0.0))
    cells = jnp.concatenate(cells, axis=0).astype(BF16)
    entering = dot(cells[:, 0:64], wd_v[...])
    coarse[0:8] = jnp.zeros((8, 256), F32)
    coarse[128:136] = jnp.zeros((8, 256), F32)
    coarse[8:128] = entering.astype(BF16).astype(F32)
    total = jnp.zeros((72, 256), F32)
    for p in range(3):
        for q in range(3):
            at = 8 + 24 * p + q - 1
            total += dot_t(coarse[at : at + 72].astype(BF16), kc_v[p, q])
    half_total = 0.5 * total
    leaving = coarse[32:104] + (half_total + half_total * jnp.tanh(half_total))
    blocks = []
    for k, (dr, dq) in enumerate(WIDE[3:12]):
        block = leaving[8 * k : 8 * k + 8]
        blocks.append(jnp.where(jnp.logical_and(row_ok(dr), col_ok(dq)), block, 0.0))
    leaving = jnp.concatenate(blocks, axis=0).astype(BF16)
    high, low = split2(dot_t(wu_v[...], leaving))
    for k in range(9):
        wide_up = dot(high, expand[k])
        up_b[k] = wide_up.astype(BF16)
        if k == 4:
            raised_ref[...] = wide_up + dot(low, expand[k])
    for edge, rhos in enumerate(((0, 1, 1), (1, 1, 1), (1, 1, 2))):
        rhs = jnp.concatenate([up_b[rhos[p] * 3 + q] for p in range(3) for q in range(3)], axis=0)
        s_ref[edge] = dot(w9[...], rhs)

    def finish(i, edge):
        at = i * 64 if isinstance(i, int) else pl.multiple_of(i * 64, 64)
        h = acc[pl.ds(at, 64), :] + s_ref[edge]
        one = fine[pl.ds(at + 64, 64), 0:WB].astype(F32)
        value = one + raised_ref[...] + (h + h * jnp.tanh(h))
        fine_three[pl.ds(at, 64), :] = value.astype(BF16)

    def finish_middle(i, carry):
        finish(i, 1)
        return carry

    finish(0, 0)
    finish(HB - 1, 2)
    lax.fori_loop(1, HB - 1, finish_middle, 0, unroll=True)
    for g in range(4):
        denoised = dot(wo8[...], fine_three[512 * g : 512 * g + 512, :])
        for v in range(4):
            rows = slice(8 * g, 8 * g + 8)
            out_h[v, rows, :] = station_a[v, rows, :] + station_b[rows, :] * denoised[8 * v : 8 * v + 8]


def dot_hi(w_in):
    place = lax.broadcasted_iota(jnp.int32, (4, 128), 1) % 4 == lax.broadcasted_iota(jnp.int32, (4, 128), 0)
    place = place.astype(F32).astype(BF16)
    high, middle, low = split3(w_in)
    return (dot(high, place) + dot(middle, place)) + dot(low, place)


def solution(mesh):
    n_ty = mesh.shape["ty"]
    n_rows = mesh.shape["grp"] * n_ty
    n_cols = mesh.shape["tx"]

    def on_device(noisy, w_in, kf, wd, kc, wu, kl, wo, cell, count, obs):
        w_in, wd = w_in.T, wd.T
        obs = obs.reshape(4, 1, 128)
        cell = cell.reshape(1, 1, 128)
        count = count.reshape(1, 1, 128)
        args = (noisy, w_in, kf, wd, kc, wu, kl, wo, cell, count, obs)
        vmem = pltpu.VMEM
        args = tuple(pltpu.with_memory_space_constraint(x, pltpu.HBM) for x in args)
        return pl.pallas_call(
            functools.partial(kernel, n_rows, n_cols, n_ty),
            out_shape=jax.ShapeDtypeStruct(noisy.shape, noisy.dtype),
            in_specs=[pl.BlockSpec(memory_space=pltpu.HBM)] * 11,
            out_specs=pl.BlockSpec(memory_space=pltpu.VMEM),
            scratch_shapes=[vmem(x.shape, x.dtype) for x in args]
            + [
                vmem((2, 8, WB), F32),
                vmem((2, 8, 128), F32),
                vmem((2, 8, WB), F32),
                vmem((2, 3, 8, 128), F32),
                vmem((3, 8, 128), F32),
                vmem((18, 8, 128), F32),
                vmem((4, 48, WE), F32),
                vmem((3, 576, 128), F32),
                vmem((576, WE), BF16),
                vmem((576, WE), BF16),
                vmem((4, 128, 240), BF16),
                vmem((3, 128, 256), BF16),
                vmem((64, 576), BF16),
                vmem((32, 512), BF16),
                vmem((9, 72, WB), BF16),
                vmem((34 * 64, WE), BF16),
                vmem((34 * 64, WB), BF16),
                vmem((34 * 64, WB), BF16),
                vmem((HB * 64, WB), F32),
                vmem((4, HB, WB), F32),
                vmem((HB, WB), F32),
                vmem((HB * 64, WB), BF16),
                vmem((136, 256), F32),
                vmem((9, 64, WB), BF16),
                vmem((3, 64, WB), F32),
                vmem((64, WB), F32),
                pltpu.SemaphoreType.DMA((11,)),
                pltpu.SemaphoreType.DMA((8,)),
                pltpu.SemaphoreType.DMA((8,)),
                pltpu.SemaphoreType.DMA((16,)),
                pltpu.SemaphoreType.DMA((18,)),
            ],
            compiler_params=pltpu.CompilerParams(
                collective_id=0, has_side_effects=True, vmem_limit_bytes=50*1024*1024
            ),
        )(*args)

    return jax.shard_map(
        on_device,
        mesh=mesh,
        in_specs=(
            P(None, ("grp", "ty"), "tx"),
            P(),
            P(),
            P(),
            P(),
            P(),
            P(),
            P(),
            P(("grp", "ty"), "tx", None),
            P(("grp", "ty"), "tx", None),
            P(None, ("grp", "ty"), "tx", None),
        ),
        out_specs=P(None, ("grp", "ty"), "tx"),
        check_vma=False,
    )
```

```python
import functools

import jax
import jax.numpy as jnp
from jax import lax
from jax.experimental import pallas as pl
from jax.experimental.pallas import tpu as pltpu
from jax.sharding import PartitionSpec as P

F32 = jnp.float32
BF16 = jnp.bfloat16
MESH = pl.DeviceIdType.MESH
NEAR = tuple((dr, dq) for dr in (-1, 0, 1) for dq in (-1, 0, 1) if (dr, dq) != (0, 0))
WIDE = tuple((dr, dq) for dr in (-2, -1, 0, 1, 2) for dq in (-1, 0, 1))
HB = 32
WB = 256
WE = 384
OWN = 9


def dot(a, b):
    return lax.dot_general(a, b, (((1,), (0,)), ((), ())), preferred_element_type=F32)


def dot_t(a, b):
    return lax.dot_general(a, b, (((1,), (1,)), ((), ())), preferred_element_type=F32)


def split2(x):
    high = x.astype(BF16)
    return high, (x - high.astype(F32)).astype(BF16)


def split3(x):
    high = x.astype(BF16)
    rest = x - high.astype(F32)
    middle = rest.astype(BF16)
    return high, middle, (rest - middle.astype(F32)).astype(BF16)


def kernel(
    n_rows,
    n_cols,
    n_ty,
    noisy_h, w_in_h, kf_h, wd_h, kc_h, wu_h, kl_h, wo_h, cell_h, count_h, obs_h,
    out_h,
    noisy_v, w_in_v, kf_v, wd_v, kc_v, wu_v, kl_v, wo_v, cell_v, count_v, obs_v,
    row_send, col_send, row_recv, col_recv, pool_send, pool_recv,
    ext, taps, taps_h, taps_l, a1, a2, w9, wo8, expand, fine, fine_l, fine_r, acc, edge_ref,
    station_a, station_b, fine_three, coarse, up_b, s_ref, raised_ref,
    in_sem, near_send, near_recv, wide_send, wide_recv,
):
    row = lax.axis_index("grp") * n_ty + lax.axis_index("ty")
    col = lax.axis_index("tx")

    def device(dr, dq):
        r = lax.rem(row + dr + n_rows, n_rows)
        q = lax.rem(col + dq + n_cols, n_cols)
        return (r // n_ty, lax.rem(r, n_ty), q)

    def row_ok(dr):
        return jnp.logical_and(row + dr >= 0, row + dr < n_rows)

    def col_ok(dq):
        return jnp.logical_and(col + dq >= 0, col + dq < n_cols)

    pairs = (
        (noisy_h, noisy_v), (w_in_h, w_in_v), (kf_h, kf_v), (kl_h, kl_v), (wo_h, wo_v), (cell_h, cell_v),
        (count_h, count_v), (obs_h, obs_v), (wd_h, wd_v), (wu_h, wu_v), (kc_h, kc_v),
    )
    loads = [pltpu.make_async_copy(src, dst, in_sem.at[k]) for k, (src, dst) in enumerate(pairs)]
    for load in loads:
        load.start()

    def there(dr, dq):
        if dq == 0:
            return row_ok(dr)
        return col_ok(dq) if dr == 0 else jnp.logical_and(row_ok(dr), col_ok(dq))

    barrier = pltpu.get_barrier_semaphore()
    for dr, dq in WIDE:
        if (dr, dq) != (0, 0):

            @pl.when(there(dr, dq))
            def _(dr=dr, dq=dq):
                pl.semaphore_signal(barrier, inc=1, device_id=device(dr, dq), device_id_type=MESH)


    loads[0].wait()
    for v in range(4):
        row_send[0, 2 * v : 2 * v + 2, :] = noisy_v[v, 0:2, :]
        row_send[1, 2 * v : 2 * v + 2, :] = noisy_v[v, HB - 2 : HB, :]
    first = jnp.concatenate([noisy_v[v, :, 0:128] for v in range(4)], axis=0)
    last = jnp.concatenate([noisy_v[v, :, 128:256] for v in range(4)], axis=0)
    col_send[0] = first.T[0:8, :]
    col_send[1] = last.T[120:128, :]

    above_count = jnp.minimum(row, 2)
    below_count = jnp.minimum(n_rows - 1 - row, 2)
    sides = jnp.minimum(col, 1) + jnp.minimum(n_cols - 1 - col, 1)
    pl.semaphore_wait(barrier, (above_count + below_count + 1) * (sides + 1) - 1)
    near = []
    for k, (dr, dq) in enumerate(NEAR):
        if dq == 0:
            src = row_send.at[0 if dr < 0 else 1]
            dst = row_recv.at[1 if dr < 0 else 0]
        else:
            src = col_send.at[0 if dq < 0 else 1]
            dst = col_recv.at[1 if dq < 0 else 0, 1 - dr]
        back = NEAR.index((-dr, -dq))
        near.append(
            pltpu.make_async_remote_copy(
                src_ref=src, dst_ref=dst, send_sem=near_send.at[k], recv_sem=near_recv.at[back],
                device_id=device(dr, dq), device_id_type=MESH,
            )
        )
    for copy, (dr, dq) in zip(near, NEAR):
        pl.when(there(dr, dq))(copy.start)

    for load in loads[1:]:
        load.wait()
    w_tiled = dot_hi(w_in_v[...].T)
    lane = lax.broadcasted_iota(jnp.int32, (64, 128), 1)
    zero64 = jnp.zeros((64, 64), BF16)
    kf9 = jnp.concatenate([kf_v[p, q] for p in range(3) for q in range(3)], axis=1)
    for r in range(4):
        placed = []
        for p in range(3):
            for q in range(3):
                at = 12 * (r + p) + 4 * q
                placed.append(jnp.where(jnp.logical_and(lane >= at, lane < at + 4), w_tiled, 0.0))
        placed = jnp.concatenate(placed, axis=0)
        high, middle, low = split3(placed)
        conv = 0.5 * (dot(kf9, high) + dot(kf9, middle) + dot(kf9, low))
        at = 12 * (r + 1) + 4
        lift = jnp.where(jnp.logical_and(lane >= at, lane < at + 4), w_tiled, 0.0)
        high, low = split2(jnp.concatenate([conv, lift], axis=0))
        a1[r, :, 0:80] = high[:, 0:80]
        a1[r, :, 80:160] = high[:, 0:80]
        a1[r, :, 160:240] = low[:, 0:80]
    half = [[(kl_v[p, q].astype(F32) * 0.5).astype(BF16) for q in range(3)] for p in range(3)]
    for q in range(3):
        upper = jnp.concatenate([half[0][q], half[1][q], half[2][q], zero64], axis=1)
        lower = jnp.concatenate([zero64, half[0][q], half[1][q], half[2][q]], axis=1)
        a2[q] = jnp.concatenate([upper, lower], axis=0)
    w9[...] = jnp.concatenate([half[p][q] for p in range(3) for q in range(3)], axis=1)
    pick = (lax.broadcasted_iota(jnp.int32, (32, 4), 0) // 8 == lax.broadcasted_iota(jnp.int32, (32, 4), 1))
    spread = dot(pick.astype(BF16), wo_v[...])
    spread = jnp.concatenate([spread] * 8, axis=1)
    same = lax.broadcasted_iota(jnp.int32, (32, 512), 0) % 8 == lax.broadcasted_iota(jnp.int32, (32, 512), 1) // 64
    wo8[...] = jnp.where(same, spread, 0.0).astype(BF16)
    cells = lax.broadcasted_iota(jnp.int32, (72, WB), 0)
    pixel = lax.broadcasted_iota(jnp.int32, (72, WB), 1)
    for rho in range(3):
        for q in range(3):
            want = rho * 24 + 7 + (pixel + (32 + q - 1)) // 32
            expand[rho * 3 + q] = (cells == want).astype(F32).astype(BF16)

    cell = cell_v[0]
    count = count_v[0].astype(F32)
    at_row = (lax.broadcasted_iota(jnp.int32, (HB, 128), 0) == cell // WB).astype(F32)
    at_col = (lax.broadcasted_iota(jnp.int32, (WB, 128), 0) == cell % WB).astype(F32).astype(BF16)
    reports = [at_row * (count * obs_v[v, 0]) for v in range(4)] + [at_row * count]
    parts = split3(jnp.concatenate(reports, axis=0))
    sums = dot_t(parts[0], at_col) + dot_t(parts[1], at_col) + dot_t(parts[2], at_col)
    for v in range(4):
        station_a[v] = 0.5 * noisy_v[v] + 0.25 * sums[HB * v : HB * (v + 1)]
    station_b[...] = 0.5 - 0.25 * sums[HB * 4 :]

    ext[...] = jnp.zeros_like(ext)
    for v in range(4):
        ext[v, OWN : OWN + HB, 0:WB] = noisy_v[v]

    def make_taps(start, size):
        rows = slice(12 * start, 12 * (start + size))
        for v in range(4):
            left, right = ext[v, start : start + size, 0:128], ext[v, start : start + size, 128:256]
            spot = lax.broadcasted_iota(jnp.int32, left.shape, 1)
            up = [pltpu.roll(x, 1, 1) for x in (left, right)]
            down = [pltpu.roll(x, 127, 1) for x in (left, right)]
            shifted = (
                (jnp.where(spot < 1, 0.0, up[0]), left, jnp.where(spot < 127, down[0], down[1])),
                (jnp.where(spot < 1, up[0], up[1]), right, jnp.where(spot < 127, down[1], 0.0)),
            )
            for t in range(2):
                for q in range(3):
                    taps[t, pl.ds(12 * start + 4 * q + v, size, stride=12), :] = shifted[t][q]
        for t in range(2):
            high, low = split2(taps[t, rows])
            taps_h[rows, 128 * t : 128 * t + 128] = high
            taps_l[rows, 128 * t : 128 * t + 128] = low

    def make_side_taps(start, size):
        for v in range(4):
            rows = slice(start, start + size)
            spot = lax.broadcasted_iota(jnp.int32, (size, 128), 1)
            near_columns = jnp.where(
                spot < 4, pltpu.roll(ext[v, rows, 0:128], 2, 1), pltpu.roll(ext[v, rows, 128:256], 6, 1)
            )
            inside = jnp.logical_and(spot >= 2, spot < 6)
            here = jnp.where(inside, near_columns, ext[v, rows, WB:WE])
            for q, value in enumerate((pltpu.roll(here, 1, 1), here, pltpu.roll(here, 127, 1))):
                taps[2, pl.ds(12 * start + 4 * q + v, size, stride=12), :] = value

    def side_columns(k):
        right = jnp.where(jnp.logical_and(row_ok(k - 1), col_ok(1)), col_recv[1, k], 0.0)
        left = jnp.where(jnp.logical_and(row_ok(k - 1), col_ok(-1)), col_recv[0, k], 0.0)
        place = lax.broadcasted_iota(jnp.int32, (8, 128), 0)
        both = jnp.where(place < 2, pltpu.roll(left, 2, 0), jnp.where(place >= 6, pltpu.roll(right, 6, 0), 0.0))
        return jnp.concatenate([both, jnp.zeros((120, 128), F32)], axis=0).T

    def window(at):
        high = taps_h[pl.ds(at, 80), :]
        return jnp.concatenate([high, taps_l[pl.ds(at, 80), :], high], axis=0)

    def gated(both):
        h = both[0:64]
        return both[64:128] + (h + h * jnp.tanh(h))

    def fine_row(i, rhs, gate=None):
        value = gated(dot(a1[i % 4], rhs))
        if gate is not None:
            value = value * jnp.where(gate, 1.0, 0.0)
        fine[64 * (i + 1) : 64 * (i + 2), 0:WB] = value.astype(BF16)
        return value

    make_taps(0, 48)
    middle = jnp.zeros((64, WB), F32)
    for g in range(8):
        rhs = window(96 + 48 * g)
        for r in range(4):
            if 0 < 4 * g + r < HB - 1:
                middle = middle + fine_row(4 * g + r, rhs)

    lane = lax.broadcasted_iota(jnp.int32, (64, 128), 1)
    group, spot = lane // 8, lane % 8
    gate = jnp.where(spot == 1, jnp.where(col_ok(-1), 1.0, 0.0), jnp.where(spot == 6, jnp.where(col_ok(1), 1.0, 0.0), 1.0))
    gate = gate * jnp.where(group == 8, jnp.where(row_ok(-1), 1.0, 0.0), jnp.where(group == 9, jnp.where(row_ok(1), 1.0, 0.0), 1.0))
    starts = [96 + 48 * g for g in range(8)] + [48, 480]
    tap_lane = lax.broadcasted_iota(jnp.int32, (80, 128), 1) // 8

    def side_inputs(groups, packed):
        for g in groups:
            value = taps[2, pl.ds(starts[g], 80), :]
            packed = jnp.where(tap_lane == g, value if g == 0 else pltpu.roll(value, 8 * g, 1), packed)
        high, low = split2(packed)
        return packed, jnp.concatenate([high, low, high], axis=0)

    def side_rows(r, rhs):
        value = gated(dot(a1[r], rhs)) * gate
        edge_ref[r] = value
        return value

    pixel = lax.broadcasted_iota(jnp.int32, (8, WE), 1)
    cell_of = jnp.where(pixel < WB, pixel // 32, jnp.where(pixel % 8 == 2, 0, jnp.where(pixel % 8 == 5, 7, 8)))
    cell_of = jnp.where(jnp.logical_or(pixel == 0, pixel == WB - 1), 8, cell_of)
    into = (cell_of == lax.broadcasted_iota(jnp.int32, (8, WE), 0)).astype(F32).astype(BF16)

    def sums_of(upper, upper_side, lower, lower_side):
        stack = jnp.concatenate(
            [jnp.concatenate([upper, upper_side], axis=1), jnp.concatenate([lower, lower_side], axis=1)], axis=0
        )
        high, low = split2(stack)
        return (dot_t(into, high) + dot_t(into, low)) * (1.0 / 1024.0)

    for k, (dr, dq) in enumerate(NEAR):
        if dr >= 0:
            pl.when(there(-dr, -dq))(near[k].wait_recv)
    above, beside = side_columns(0), side_columns(1)
    for v in range(4):
        ext[v, OWN - 2 : OWN, 0:WB] = jnp.where(row_ok(-1), row_recv[0, 2 * v : 2 * v + 2, :], 0.0)
        ext[v, OWN - 2 : OWN, WB:WE] = above[HB * v + HB - 2 : HB * v + HB]
        ext[v, OWN : OWN + HB, WB:WE] = beside[HB * v : HB * (v + 1)]
    make_taps(0, 16)
    make_side_taps(0, 48)
    first_row = fine_row(0, window(96))
    outer_row = fine_row(-1, window(48), row_ok(-1))
    packed, rhs = side_inputs(range(10), jnp.zeros((80, 128), F32))
    side = [side_rows(r, rhs) for r in range(4)]
    inner_side = jnp.where(lane < 64, side[1] + side[2], 0.0)
    side_sum = inner_side + jnp.where(lane < 64, side[0], 0.0) + jnp.where(lane < 56, side[3], 0.0)
    outer_side = jnp.where(group == 8, side[3], 0.0)
    tile = sums_of(middle + first_row, side_sum, outer_row, outer_side)
    pool_send[0] = tile
    wide, wide_at = [], []

    def send(which, dr, dq, slot):
        wide.append(
            pltpu.make_async_remote_copy(
                src_ref=pool_send.at[which], dst_ref=pool_recv.at[slot], send_sem=wide_send.at[len(wide)],
                recv_sem=wide_recv.at[slot], device_id=device(dr, dq), device_id_type=MESH,
            )
        )
        pl.when(there(dr, dq))(wide[-1].start)
        wide_at.append((dr, dq))

    for dr in (1, 2):
        for dq in (-1, 0, 1):
            send(0, dr, dq, WIDE.index((-dr, -dq)))
    for dq in (-1, 1):
        send(0, 0, dq, WIDE.index((0, -dq)))
    pool_recv[WIDE.index((0, 0))] = tile

    for k, (dr, dq) in enumerate(NEAR):
        if dr < 0:
            pl.when(there(-dr, -dq))(near[k].wait_recv)
    below = side_columns(2)
    for v in range(4):
        ext[v, OWN + HB : OWN + HB + 2, 0:WB] = jnp.where(row_ok(1), row_recv[1, 2 * v : 2 * v + 2, :], 0.0)
        ext[v, OWN + HB : OWN + HB + 2, WB:WE] = below[HB * v : HB * v + 2]
    make_taps(40, 8)
    make_side_taps(40, 8)
    last_row = fine_row(HB - 1, window(432))
    outer_row = fine_row(HB, window(480), row_ok(1))
    packed, rhs = side_inputs((7, 9), packed)
    low_side, top_side = side_rows(3, rhs), side_rows(0, rhs)
    outer_side = jnp.where(group == 9, top_side, 0.0)
    inner_side = inner_side + jnp.where(lane < 64, low_side, 0.0)
    all_side = inner_side + jnp.where(lane < 64, top_side, 0.0)
    low_sum = inner_side + jnp.where(jnp.logical_and(lane >= 8, lane < 64), top_side, 0.0)
    pool_send[1] = sums_of(middle + last_row, low_sum, outer_row, outer_side)
    tile = sums_of(middle + first_row + last_row, all_side, outer_row, outer_side)
    pool_send[2] = tile
    for dr in (-1, -2):
        for dq in (-1, 0, 1):
            send(1, dr, dq, WIDE.index((-dr, -dq)))
    for dq in (-1, 1):
        send(2, 0, dq, 16 - dq)
    pool_recv[16] = tile

    for e in range(HB + 2):
        g = 8 if e == 0 else 9 if e == HB + 1 else (e - 1) // 4
        edge = edge_ref[(e - 1) % 4]
        rows = slice(64 * e, 64 * e + 64)
        left, right = fine[rows, 0:128].astype(F32), fine[rows, 128:256].astype(F32)
        up = [pltpu.roll(x, 1, 1) for x in (left, right)]
        down = [pltpu.roll(x, 127, 1) for x in (left, right)]
        turned = [pltpu.roll(edge, (at - 8 * g) % 128, 1) for at in (-1, -2, 122, 121)]
        fine_l[rows, 0:128] = jnp.where(lane < 2, turned[0], up[0]).astype(BF16)
        fine_l[rows, 128:256] = jnp.where(lane < 1, up[0], up[1]).astype(BF16)
        fine_r[rows, 0:128] = jnp.where(lane < 127, down[0], down[1]).astype(BF16)
        fine_r[rows, 128:256] = jnp.where(lane < 126, down[1], turned[3]).astype(BF16)
        fine[rows, 0:128] = jnp.where(lane < 1, turned[1], left).astype(BF16)
        fine[rows, 128:256] = jnp.where(lane < 127, right, turned[2]).astype(BF16)

    def last_rows(k, carry):
        at = pl.multiple_of(k * 128, 128)
        total = dot(a2[0], fine_l[pl.ds(at, 256), :])
        total += dot(a2[1], fine[pl.ds(at, 256), 0:WB])
        total += dot(a2[2], fine_r[pl.ds(at, 256), :])
        acc[pl.ds(at, 128), :] = total
        return carry

    lax.fori_loop(0, 16, last_rows, 0, unroll=True)

    for copy, (dr, dq) in zip(wide, wide_at):
        pl.when(there(-dr, -dq))(copy.wait_recv)
    for copy, (dr, dq) in zip(wide + near, wide_at + list(NEAR)):
        pl.when(there(dr, dq))(copy.wait_send)
    cells = []
    for dr, dq in WIDE:
        if dr == 0:
            cell = pool_recv[16 + dq]
        else:
            step = 1 if dr > 0 else -1
            if dr == 1:
                other = pool_recv[16 + dq]
            else:
                other = pool_recv[WIDE.index((dr - step, dq))]
            cell = pool_recv[WIDE.index((dr, dq))] + pltpu.roll(other, 64, 1)
        cells.append(jnp.where(jnp.logical_and(row_ok(dr), col_ok(dq)), cell, 0.0))
    cells = jnp.concatenate(cells, axis=0).astype(BF16)
    entering = dot(cells[:, 0:64], wd_v[...])
    coarse[0:8] = jnp.zeros((8, 256), F32)
    coarse[128:136] = jnp.zeros((8, 256), F32)
    coarse[8:128] = entering.astype(BF16).astype(F32)
    total = jnp.zeros((72, 256), F32)
    for p in range(3):
        for q in range(3):
            at = 8 + 24 * p + q - 1
            total += dot_t(coarse[at : at + 72].astype(BF16), kc_v[p, q])
    half_total = 0.5 * total
    leaving = coarse[32:104] + (half_total + half_total * jnp.tanh(half_total))
    blocks = []
    for k, (dr, dq) in enumerate(WIDE[3:12]):
        block = leaving[8 * k : 8 * k + 8]
        blocks.append(jnp.where(jnp.logical_and(row_ok(dr), col_ok(dq)), block, 0.0))
    leaving = jnp.concatenate(blocks, axis=0).astype(BF16)
    high, low = split2(dot_t(wu_v[...], leaving))
    for k in range(9):
        wide_up = dot(high, expand[k])
        up_b[k] = wide_up.astype(BF16)
        if k == 4:
            raised_ref[...] = wide_up + dot(low, expand[k])
    for edge, rhos in enumerate(((0, 1, 1), (1, 1, 1), (1, 1, 2))):
        rhs = jnp.concatenate([up_b[rhos[p] * 3 + q] for p in range(3) for q in range(3)], axis=0)
        s_ref[edge] = dot(w9[...], rhs)

    def finish(i, edge):
        at = i * 64 if isinstance(i, int) else pl.multiple_of(i * 64, 64)
        h = acc[pl.ds(at, 64), :] + s_ref[edge]
        one = fine[pl.ds(at + 64, 64), 0:WB].astype(F32)
        value = one + raised_ref[...] + (h + h * jnp.tanh(h))
        fine_three[pl.ds(at, 64), :] = value.astype(BF16)

    def finish_middle(i, carry):
        finish(i, 1)
        return carry

    finish(0, 0)
    finish(HB - 1, 2)
    lax.fori_loop(1, HB - 1, finish_middle, 0, unroll=True)
    for g in range(4):
        denoised = dot(wo8[...], fine_three[512 * g : 512 * g + 512, :])
        for v in range(4):
            rows = slice(8 * g, 8 * g + 8)
            out_h[v, rows, :] = station_a[v, rows, :] + station_b[rows, :] * denoised[8 * v : 8 * v + 8]


def dot_hi(w_in):
    place = lax.broadcasted_iota(jnp.int32, (4, 128), 1) % 4 == lax.broadcasted_iota(jnp.int32, (4, 128), 0)
    place = place.astype(F32).astype(BF16)
    high, middle, low = split3(w_in)
    return (dot(high, place) + dot(middle, place)) + dot(low, place)


def solution(mesh):
    n_ty = mesh.shape["ty"]
    n_rows = mesh.shape["grp"] * n_ty
    n_cols = mesh.shape["tx"]

    def on_device(noisy, w_in, kf, wd, kc, wu, kl, wo, cell, count, obs):
        w_in, wd = w_in.T, wd.T
        obs = obs.reshape(4, 1, 128)
        cell = cell.reshape(1, 1, 128)
        count = count.reshape(1, 1, 128)
        args = (noisy, w_in, kf, wd, kc, wu, kl, wo, cell, count, obs)
        vmem = pltpu.VMEM
        args = tuple(pltpu.with_memory_space_constraint(x, pltpu.HBM) for x in args)
        return pl.pallas_call(
            functools.partial(kernel, n_rows, n_cols, n_ty),
            out_shape=jax.ShapeDtypeStruct(noisy.shape, noisy.dtype),
            in_specs=[pl.BlockSpec(memory_space=pltpu.HBM)] * 11,
            out_specs=pl.BlockSpec(memory_space=pltpu.VMEM),
            scratch_shapes=[vmem(x.shape, x.dtype) for x in args]
            + [
                vmem((2, 8, WB), F32),
                vmem((2, 8, 128), F32),
                vmem((2, 8, WB), F32),
                vmem((2, 3, 8, 128), F32),
                vmem((3, 8, 128), F32),
                vmem((18, 8, 128), F32),
                vmem((4, 48, WE), F32),
                vmem((3, 576, 128), F32),
                vmem((576, WB), BF16),
                vmem((576, WB), BF16),
                vmem((4, 128, 240), BF16),
                vmem((3, 128, 256), BF16),
                vmem((64, 576), BF16),
                vmem((32, 512), BF16),
                vmem((9, 72, WB), BF16),
                vmem((34 * 64, WB), BF16),
                vmem((34 * 64, WB), BF16),
                vmem((34 * 64, WB), BF16),
                vmem((HB * 64, WB), F32),
                vmem((4, 64, 128), F32),
                vmem((4, HB, WB), F32),
                vmem((HB, WB), F32),
                vmem((HB * 64, WB), BF16),
                vmem((136, 256), F32),
                vmem((9, 64, WB), BF16),
                vmem((3, 64, WB), F32),
                vmem((64, WB), F32),
                pltpu.SemaphoreType.DMA((11,)),
                pltpu.SemaphoreType.DMA((8,)),
                pltpu.SemaphoreType.DMA((8,)),
                pltpu.SemaphoreType.DMA((16,)),
                pltpu.SemaphoreType.DMA((18,)),
            ],
            compiler_params=pltpu.CompilerParams(
                collective_id=0, has_side_effects=True, vmem_limit_bytes=50*1024*1024
            ),
        )(*args)

    return jax.shard_map(
        on_device,
        mesh=mesh,
        in_specs=(
            P(None, ("grp", "ty"), "tx"),
            P(),
            P(),
            P(),
            P(),
            P(),
            P(),
            P(),
            P(("grp", "ty"), "tx", None),
            P(("grp", "ty"), "tx", None),
            P(None, ("grp", "ty"), "tx", None),
        ),
        out_specs=P(None, ("grp", "ty"), "tx"),
        check_vma=False,
    )
```

```python
import functools

import jax
import jax.numpy as jnp
from jax import lax
from jax.experimental import pallas as pl
from jax.experimental.pallas import tpu as pltpu
from jax.sharding import PartitionSpec as P

F32 = jnp.float32
BF16 = jnp.bfloat16
MESH = pl.DeviceIdType.MESH
NEAR = tuple((dr, dq) for dr in (-1, 0, 1) for dq in (-1, 0, 1) if (dr, dq) != (0, 0))
WIDE = tuple((dr, dq) for dr in (-2, -1, 0, 1, 2) for dq in (-1, 0, 1))
HB = 32
WB = 256
WE = 384
OWN = 9


def dot(a, b):
    return lax.dot_general(a, b, (((1,), (0,)), ((), ())), preferred_element_type=F32)


def dot_t(a, b):
    return lax.dot_general(a, b, (((1,), (1,)), ((), ())), preferred_element_type=F32)


def split2(x):
    high = x.astype(BF16)
    return high, (x - high.astype(F32)).astype(BF16)


def split3(x):
    high = x.astype(BF16)
    rest = x - high.astype(F32)
    middle = rest.astype(BF16)
    return high, middle, (rest - middle.astype(F32)).astype(BF16)


def kernel(
    n_rows,
    n_cols,
    n_ty,
    noisy_h, w_in_h, kf_h, wd_h, kc_h, wu_h, kl_h, wo_h, cell_h, count_h, obs_h,
    out_h,
    noisy_v, w_in_v, kf_v, wd_v, kc_v, wu_v, kl_v, wo_v, cell_v, count_v, obs_v,
    row_send, col_send, row_recv, col_recv, pool_send, pool_recv,
    ext, taps, taps_h, taps_l, a1, a2, enter_w, leave_w, wo8, expand, fine, fine_l, fine_r, acc, edge_ref,
    station_a, station_b, fine_three, coarse, s_ref, raised_ref,
    in_sem, near_send, near_recv, wide_send, wide_recv,
):
    row = lax.axis_index("grp") * n_ty + lax.axis_index("ty")
    col = lax.axis_index("tx")

    row_of = {dr: (lax.div(row + dr, n_ty), lax.rem(row + dr, n_ty)) for dr in range(-2, 3)}

    def device(dr, dq):
        return row_of[dr] + (col + dq,)

    def row_ok(dr):
        return jnp.logical_and(row + dr >= 0, row + dr < n_rows)

    def col_ok(dq):
        return jnp.logical_and(col + dq >= 0, col + dq < n_cols)

    pairs = (
        (noisy_h, noisy_v), (w_in_h, w_in_v), (kf_h, kf_v), (kl_h, kl_v), (wo_h, wo_v), (cell_h, cell_v),
        (count_h, count_v), (obs_h, obs_v), (wd_h, wd_v), (wu_h, wu_v), (kc_h, kc_v),
    )
    loads = [pltpu.make_async_copy(src, dst, in_sem.at[k]) for k, (src, dst) in enumerate(pairs)]
    for load in loads:
        load.start()

    def there(dr, dq):
        if dq == 0:
            return row_ok(dr)
        return col_ok(dq) if dr == 0 else jnp.logical_and(row_ok(dr), col_ok(dq))

    barrier = pltpu.get_barrier_semaphore()
    for dr, dq in WIDE:
        if (dr, dq) != (0, 0):

            @pl.when(there(dr, dq))
            def _(dr=dr, dq=dq):
                pl.semaphore_signal(barrier, inc=1, device_id=device(dr, dq), device_id_type=MESH)


    loads[0].wait()
    for v in range(4):
        row_send[0, 2 * v : 2 * v + 2, :] = noisy_v[v, 0:2, :]
        row_send[1, 2 * v : 2 * v + 2, :] = noisy_v[v, HB - 2 : HB, :]
    first = jnp.concatenate([noisy_v[v, :, 0:128] for v in range(4)], axis=0)
    last = jnp.concatenate([noisy_v[v, :, 128:256] for v in range(4)], axis=0)
    col_send[0] = first.T[0:8, :]
    col_send[1] = last.T[120:128, :]

    above_count = jnp.minimum(row, 2)
    below_count = jnp.minimum(n_rows - 1 - row, 2)
    sides = jnp.minimum(col, 1) + jnp.minimum(n_cols - 1 - col, 1)
    pl.semaphore_wait(barrier, (above_count + below_count + 1) * (sides + 1) - 1)
    near = []
    for k, (dr, dq) in enumerate(NEAR):
        if dq == 0:
            src = row_send.at[0 if dr < 0 else 1]
            dst = row_recv.at[1 if dr < 0 else 0]
        else:
            src = col_send.at[0 if dq < 0 else 1]
            dst = col_recv.at[1 if dq < 0 else 0, 1 - dr]
        back = NEAR.index((-dr, -dq))
        near.append(
            pltpu.make_async_remote_copy(
                src_ref=src, dst_ref=dst, send_sem=near_send.at[k], recv_sem=near_recv.at[back],
                device_id=device(dr, dq), device_id_type=MESH,
            )
        )
    for copy, (dr, dq) in zip(near, NEAR):
        pl.when(there(dr, dq))(copy.start)

    for load in loads[1:]:
        load.wait()
    w_tiled = dot_hi(w_in_v[...].T)
    lane = lax.broadcasted_iota(jnp.int32, (64, 128), 1)
    zero64 = jnp.zeros((64, 64), BF16)
    kf9 = jnp.concatenate([kf_v[p, q] for p in range(3) for q in range(3)], axis=1)
    for r in range(4):
        placed = []
        for p in range(3):
            for q in range(3):
                at = 12 * (r + p) + 4 * q
                placed.append(jnp.where(jnp.logical_and(lane >= at, lane < at + 4), w_tiled, 0.0))
        placed = jnp.concatenate(placed, axis=0)
        high, middle, low = split3(placed)
        conv = 0.5 * (dot(kf9, high) + dot(kf9, middle) + dot(kf9, low))
        at = 12 * (r + 1) + 4
        lift = jnp.where(jnp.logical_and(lane >= at, lane < at + 4), w_tiled, 0.0)
        high, low = split2(jnp.concatenate([conv, lift], axis=0))
        a1[r, :, 0:80] = high[:, 0:80]
        a1[r, :, 80:160] = high[:, 0:80]
        a1[r, :, 160:240] = low[:, 0:80]
    half = [[(kl_v[p, q].astype(F32) * 0.5).astype(BF16) for q in range(3)] for p in range(3)]
    for q in range(3):
        upper = jnp.concatenate([half[0][q], half[1][q], half[2][q], zero64], axis=1)
        lower = jnp.concatenate([zero64, half[0][q], half[1][q], half[2][q]], axis=1)
        a2[q] = jnp.concatenate([upper, lower], axis=0)
    stack = jnp.concatenate([half[p][q] for p in range(3) for q in range(3)], axis=0)
    leave_w[0:576] = dot(stack, wu_v[...]).astype(BF16)
    leave_w[576:640] = wu_v[...]
    down = jnp.concatenate([wd_v[...], jnp.zeros((64, 256), BF16)], axis=0)
    for p in range(3):
        for q in range(3):
            at = 128 * (3 * p + q)
            enter_w[at : at + 128] = dot_t(down, kc_v[p, q]).astype(BF16)
    pick = (lax.broadcasted_iota(jnp.int32, (32, 4), 0) // 8 == lax.broadcasted_iota(jnp.int32, (32, 4), 1))
    spread = dot(pick.astype(BF16), wo_v[...])
    spread = jnp.concatenate([spread] * 8, axis=1)
    same = lax.broadcasted_iota(jnp.int32, (32, 512), 0) % 8 == lax.broadcasted_iota(jnp.int32, (32, 512), 1) // 64
    wo8[...] = jnp.where(same, spread, 0.0).astype(BF16)
    place = lax.broadcasted_iota(jnp.int32, (128, WB), 0)
    pixel = lax.broadcasted_iota(jnp.int32, (128, WB), 1)
    for q in range(3):
        want = 7 + (pixel + (32 + q - 1)) // 32
        found = jnp.logical_and(place < 72, place % 24 == want)
        expand[128 * q : 128 * q + 128] = found.astype(F32).astype(BF16)

    cell = cell_v[0]
    count = count_v[0].astype(F32)
    at_row = (lax.broadcasted_iota(jnp.int32, (HB, 128), 0) == cell // WB).astype(F32)
    at_col = (lax.broadcasted_iota(jnp.int32, (WB, 128), 0) == cell % WB).astype(F32).astype(BF16)
    reports = [at_row * (count * obs_v[v, 0]) for v in range(4)] + [at_row * count]
    parts = split3(jnp.concatenate(reports, axis=0))
    sums = dot_t(parts[0], at_col) + dot_t(parts[1], at_col) + dot_t(parts[2], at_col)
    for v in range(4):
        station_a[v] = 0.5 * noisy_v[v] + 0.25 * sums[HB * v : HB * (v + 1)]
    station_b[...] = 0.5 - 0.25 * sums[HB * 4 :]

    ext[...] = jnp.zeros_like(ext)
    for v in range(4):
        ext[v, OWN : OWN + HB, 0:WB] = noisy_v[v]

    def make_taps(start, size):
        rows = slice(12 * start, 12 * (start + size))
        for v in range(4):
            left, right = ext[v, start : start + size, 0:128], ext[v, start : start + size, 128:256]
            spot = lax.broadcasted_iota(jnp.int32, left.shape, 1)
            up = [pltpu.roll(x, 1, 1) for x in (left, right)]
            down = [pltpu.roll(x, 127, 1) for x in (left, right)]
            shifted = (
                (jnp.where(spot < 1, 0.0, up[0]), left, jnp.where(spot < 127, down[0], down[1])),
                (jnp.where(spot < 1, up[0], up[1]), right, jnp.where(spot < 127, down[1], 0.0)),
            )
            for t in range(2):
                for q in range(3):
                    taps[t, pl.ds(12 * start + 4 * q + v, size, stride=12), :] = shifted[t][q]
        for t in range(2):
            high, low = split2(taps[t, rows])
            taps_h[rows, 128 * t : 128 * t + 128] = high
            taps_l[rows, 128 * t : 128 * t + 128] = low

    def make_side_taps(start, size):
        for v in range(4):
            rows = slice(start, start + size)
            spot = lax.broadcasted_iota(jnp.int32, (size, 128), 1)
            near_columns = jnp.where(
                spot < 4, pltpu.roll(ext[v, rows, 0:128], 2, 1), pltpu.roll(ext[v, rows, 128:256], 6, 1)
            )
            inside = jnp.logical_and(spot >= 2, spot < 6)
            here = jnp.where(inside, near_columns, ext[v, rows, WB:WE])
            for q, value in enumerate((pltpu.roll(here, 1, 1), here, pltpu.roll(here, 127, 1))):
                taps[2, pl.ds(12 * start + 4 * q + v, size, stride=12), :] = value

    def side_columns(k):
        right = jnp.where(jnp.logical_and(row_ok(k - 1), col_ok(1)), col_recv[1, k], 0.0)
        left = jnp.where(jnp.logical_and(row_ok(k - 1), col_ok(-1)), col_recv[0, k], 0.0)
        place = lax.broadcasted_iota(jnp.int32, (8, 128), 0)
        both = jnp.where(place < 2, pltpu.roll(left, 2, 0), jnp.where(place >= 6, pltpu.roll(right, 6, 0), 0.0))
        return jnp.concatenate([both, jnp.zeros((120, 128), F32)], axis=0).T

    def window(at):
        high = taps_h[pl.ds(at, 80), :]
        return jnp.concatenate([high, taps_l[pl.ds(at, 80), :], high], axis=0)

    def gated(both):
        h = both[0:64]
        return both[64:128] + (h + h * jnp.tanh(h))

    def fine_row(i, rhs, gate=None):
        value = gated(dot(a1[i % 4], rhs))
        if gate is not None:
            value = value * jnp.where(gate, 1.0, 0.0)
        fine[64 * (i + 1) : 64 * (i + 2), 0:WB] = value.astype(BF16)
        return value

    make_taps(0, 48)
    middle = jnp.zeros((64, WB), F32)
    for g in range(8):
        rhs = window(96 + 48 * g)
        for r in range(4):
            if 0 < 4 * g + r < HB - 1:
                middle = middle + fine_row(4 * g + r, rhs)

    lane = lax.broadcasted_iota(jnp.int32, (64, 128), 1)
    group, spot = lane // 8, lane % 8
    gate = jnp.where(spot == 1, jnp.where(col_ok(-1), 1.0, 0.0), jnp.where(spot == 6, jnp.where(col_ok(1), 1.0, 0.0), 1.0))
    gate = gate * jnp.where(group == 8, jnp.where(row_ok(-1), 1.0, 0.0), jnp.where(group == 9, jnp.where(row_ok(1), 1.0, 0.0), 1.0))
    starts = [96 + 48 * g for g in range(8)] + [48, 480]
    tap_lane = lax.broadcasted_iota(jnp.int32, (80, 128), 1) // 8

    def side_inputs(groups, packed):
        for g in groups:
            value = taps[2, pl.ds(starts[g], 80), :]
            packed = jnp.where(tap_lane == g, value if g == 0 else pltpu.roll(value, 8 * g, 1), packed)
        high, low = split2(packed)
        return packed, jnp.concatenate([high, low, high], axis=0)

    def side_rows(r, rhs):
        value = gated(dot(a1[r], rhs)) * gate
        edge_ref[r] = value
        return value

    pixel = lax.broadcasted_iota(jnp.int32, (8, WE), 1)
    cell_of = jnp.where(pixel < WB, pixel // 32, jnp.where(pixel % 8 == 2, 0, jnp.where(pixel % 8 == 5, 7, 8)))
    cell_of = jnp.where(jnp.logical_or(pixel == 0, pixel == WB - 1), 8, cell_of)
    into = (cell_of == lax.broadcasted_iota(jnp.int32, (8, WE), 0)).astype(F32).astype(BF16)

    def sums_of(upper, upper_side, lower, lower_side):
        stack = jnp.concatenate(
            [jnp.concatenate([upper, upper_side], axis=1), jnp.concatenate([lower, lower_side], axis=1)], axis=0
        )
        high, low = split2(stack)
        return (dot_t(into, high) + dot_t(into, low)) * (1.0 / 1024.0)

    for k, (dr, dq) in enumerate(NEAR):
        if dr >= 0:
            pl.when(there(-dr, -dq))(near[k].wait_recv)
    above, beside = side_columns(0), side_columns(1)
    for v in range(4):
        ext[v, OWN - 2 : OWN, 0:WB] = jnp.where(row_ok(-1), row_recv[0, 2 * v : 2 * v + 2, :], 0.0)
        ext[v, OWN - 2 : OWN, WB:WE] = above[HB * v + HB - 2 : HB * v + HB]
        ext[v, OWN : OWN + HB, WB:WE] = beside[HB * v : HB * (v + 1)]
    make_taps(0, 16)
    make_side_taps(0, 48)
    first_row = fine_row(0, window(96))
    outer_row = fine_row(-1, window(48), row_ok(-1))
    packed, rhs = side_inputs(range(10), jnp.zeros((80, 128), F32))
    side = [side_rows(r, rhs) for r in range(4)]
    inner_side = jnp.where(lane < 64, side[1] + side[2], 0.0)
    side_sum = inner_side + jnp.where(lane < 64, side[0], 0.0) + jnp.where(lane < 56, side[3], 0.0)
    outer_side = jnp.where(group == 8, side[3], 0.0)
    tile = sums_of(middle + first_row, side_sum, outer_row, outer_side)
    pool_send[0] = tile
    wide, wide_at = [], []

    def send(which, dr, dq, slot):
        wide.append(
            pltpu.make_async_remote_copy(
                src_ref=pool_send.at[which], dst_ref=pool_recv.at[slot], send_sem=wide_send.at[len(wide)],
                recv_sem=wide_recv.at[slot], device_id=device(dr, dq), device_id_type=MESH,
            )
        )
        pl.when(there(dr, dq))(wide[-1].start)
        wide_at.append((dr, dq))

    for dr in (1, 2):
        for dq in (-1, 0, 1):
            send(0, dr, dq, WIDE.index((-dr, -dq)))
    for dq in (-1, 1):
        send(0, 0, dq, WIDE.index((0, -dq)))
    pool_recv[WIDE.index((0, 0))] = tile

    for k, (dr, dq) in enumerate(NEAR):
        if dr < 0:
            pl.when(there(-dr, -dq))(near[k].wait_recv)
    below = side_columns(2)
    for v in range(4):
        ext[v, OWN + HB : OWN + HB + 2, 0:WB] = jnp.where(row_ok(1), row_recv[1, 2 * v : 2 * v + 2, :], 0.0)
        ext[v, OWN + HB : OWN + HB + 2, WB:WE] = below[HB * v : HB * v + 2]
    make_taps(40, 8)
    make_side_taps(40, 8)
    last_row = fine_row(HB - 1, window(432))
    outer_row = fine_row(HB, window(480), row_ok(1))
    packed, rhs = side_inputs((7, 9), packed)
    low_side, top_side = side_rows(3, rhs), side_rows(0, rhs)
    outer_side = jnp.where(group == 9, top_side, 0.0)
    inner_side = inner_side + jnp.where(lane < 64, low_side, 0.0)
    all_side = inner_side + jnp.where(lane < 64, top_side, 0.0)
    low_sum = inner_side + jnp.where(jnp.logical_and(lane >= 8, lane < 64), top_side, 0.0)
    pool_send[1] = sums_of(middle + last_row, low_sum, outer_row, outer_side)
    tile = sums_of(middle + first_row + last_row, all_side, outer_row, outer_side)
    pool_send[2] = tile
    for dr in (-1, -2):
        for dq in (-1, 0, 1):
            send(1, dr, dq, WIDE.index((-dr, -dq)))
    for dq in (-1, 1):
        send(2, 0, dq, 16 - dq)
    pool_recv[16] = tile

    for e in range(HB + 2):
        g = 8 if e == 0 else 9 if e == HB + 1 else (e - 1) // 4
        edge = edge_ref[(e - 1) % 4]
        rows = slice(64 * e, 64 * e + 64)
        left, right = fine[rows, 0:128].astype(F32), fine[rows, 128:256].astype(F32)
        up = [pltpu.roll(x, 1, 1) for x in (left, right)]
        down = [pltpu.roll(x, 127, 1) for x in (left, right)]
        turned = [pltpu.roll(edge, (at - 8 * g) % 128, 1) for at in (-1, -2, 122, 121)]
        fine_l[rows, 0:128] = jnp.where(lane < 2, turned[0], up[0]).astype(BF16)
        fine_l[rows, 128:256] = jnp.where(lane < 1, up[0], up[1]).astype(BF16)
        fine_r[rows, 0:128] = jnp.where(lane < 127, down[0], down[1]).astype(BF16)
        fine_r[rows, 128:256] = jnp.where(lane < 126, down[1], turned[3]).astype(BF16)
        fine[rows, 0:128] = jnp.where(lane < 1, turned[1], left).astype(BF16)
        fine[rows, 128:256] = jnp.where(lane < 127, right, turned[2]).astype(BF16)

    def last_rows(k, carry):
        at = pl.multiple_of(k * 128, 128)
        total = dot(a2[0], fine_l[pl.ds(at, 256), :])
        total += dot(a2[1], fine[pl.ds(at, 256), 0:WB])
        total += dot(a2[2], fine_r[pl.ds(at, 256), :])
        acc[pl.ds(at, 128), :] = total
        return carry

    lax.fori_loop(0, 16, last_rows, 0, unroll=True)

    for copy, (dr, dq) in zip(wide, wide_at):
        pl.when(there(-dr, -dq))(copy.wait_recv)
    for copy, (dr, dq) in zip(wide + near, wide_at + list(NEAR)):
        pl.when(there(dr, dq))(copy.wait_send)
    cells = []
    for dr, dq in WIDE:
        if dr == 0:
            cell = pool_recv[16 + dq]
        else:
            step = 1 if dr > 0 else -1
            if dr == 1:
                other = pool_recv[16 + dq]
            else:
                other = pool_recv[WIDE.index((dr - step, dq))]
            cell = pool_recv[WIDE.index((dr, dq))] + pltpu.roll(other, 64, 1)
        cells.append(jnp.where(jnp.logical_and(row_ok(dr), col_ok(dq)), cell, 0.0))
    cells = jnp.concatenate(cells, axis=0)
    coarse[0:8] = jnp.zeros((8, 128), F32)
    coarse[128:136] = jnp.zeros((8, 128), F32)
    coarse[8:128] = cells
    around = jnp.concatenate(
        [coarse[8 + 24 * p + q - 1 : 80 + 24 * p + q - 1].astype(BF16) for p in range(3) for q in range(3)], axis=1
    )
    h = 0.5 * dot(around, enter_w[...])
    leaving = dot(cells[24:96, 0:64].astype(BF16), wd_v[...]) + (h + h * jnp.tanh(h))
    blocks = []
    for k, (dr, dq) in enumerate(WIDE[3:12]):
        block = leaving[8 * k : 8 * k + 8]
        blocks.append(jnp.where(jnp.logical_and(row_ok(dr), col_ok(dq)), block, 0.0))
    leaving = jnp.concatenate(blocks + [jnp.zeros((56, 256), F32)], axis=0).astype(BF16)
    parts = dot_t(leave_w[...], leaving)
    cell_lane = lax.broadcasted_iota(jnp.int32, (64, 128), 1)
    inside = jnp.logical_and(cell_lane >= 24, cell_lane < 48)
    mixed = []
    raised = jnp.where(inside, parts[576:640], 0.0)
    none = jnp.zeros((64, 128), F32)
    raised_low = raised - raised.astype(BF16).astype(F32)
    for q in range(3):
        one, two, three = (parts[64 * (3 * p + q) : 64 * (3 * p + q) + 64] for p in range(3))
        mixed.append(
            jnp.concatenate(
                [
                    jnp.where(cell_lane < 24, one, jnp.where(inside, two + three, 0.0)),
                    jnp.where(inside, one + two + three, 0.0),
                    jnp.where(inside, one + two, jnp.where(cell_lane >= 48, three, 0.0)),
                    raised if q == 1 else none,
                    raised_low if q == 1 else none,
                ],
                axis=0,
            ).astype(BF16)
        )
    spread = dot(jnp.concatenate(mixed, axis=1), expand[...])
    for edge in range(3):
        s_ref[edge] = spread[64 * edge : 64 * edge + 64]
    raised_ref[...] = spread[192:256] + spread[256:320]

    def finish(i, edge):
        at = i * 64 if isinstance(i, int) else pl.multiple_of(i * 64, 64)
        h = acc[pl.ds(at, 64), :] + s_ref[edge]
        one = fine[pl.ds(at + 64, 64), 0:WB].astype(F32)
        value = one + raised_ref[...] + (h + h * jnp.tanh(h))
        fine_three[pl.ds(at, 64), :] = value.astype(BF16)

    def finish_middle(i, carry):
        finish(i, 1)
        return carry

    finish(0, 0)
    finish(HB - 1, 2)
    lax.fori_loop(1, HB - 1, finish_middle, 0, unroll=True)
    for g in range(4):
        denoised = dot(wo8[...], fine_three[512 * g : 512 * g + 512, :])
        for v in range(4):
            rows = slice(8 * g, 8 * g + 8)
            out_h[v, rows, :] = station_a[v, rows, :] + station_b[rows, :] * denoised[8 * v : 8 * v + 8]


def dot_hi(w_in):
    place = lax.broadcasted_iota(jnp.int32, (4, 128), 1) % 4 == lax.broadcasted_iota(jnp.int32, (4, 128), 0)
    place = place.astype(F32).astype(BF16)
    high, middle, low = split3(w_in)
    return (dot(high, place) + dot(middle, place)) + dot(low, place)


def solution(mesh):
    n_ty = mesh.shape["ty"]
    n_rows = mesh.shape["grp"] * n_ty
    n_cols = mesh.shape["tx"]

    def on_device(noisy, w_in, kf, wd, kc, wu, kl, wo, cell, count, obs):
        w_in, wd = w_in.T, wd.T
        obs = obs.reshape(4, 1, 128)
        cell = cell.reshape(1, 1, 128)
        count = count.reshape(1, 1, 128)
        args = (noisy, w_in, kf, wd, kc, wu, kl, wo, cell, count, obs)
        vmem = pltpu.VMEM
        args = tuple(pltpu.with_memory_space_constraint(x, pltpu.HBM) for x in args)
        return pl.pallas_call(
            functools.partial(kernel, n_rows, n_cols, n_ty),
            out_shape=jax.ShapeDtypeStruct(noisy.shape, noisy.dtype),
            in_specs=[pl.BlockSpec(memory_space=pltpu.HBM)] * 11,
            out_specs=pl.BlockSpec(memory_space=pltpu.VMEM),
            scratch_shapes=[vmem(x.shape, x.dtype) for x in args]
            + [
                vmem((2, 8, WB), F32),
                vmem((2, 8, 128), F32),
                vmem((2, 8, WB), F32),
                vmem((2, 3, 8, 128), F32),
                vmem((3, 8, 128), F32),
                vmem((18, 8, 128), F32),
                vmem((4, 48, WE), F32),
                vmem((3, 576, 128), F32),
                vmem((576, WB), BF16),
                vmem((576, WB), BF16),
                vmem((4, 128, 240), BF16),
                vmem((3, 128, 256), BF16),
                vmem((1152, 256), BF16),
                vmem((640, 256), BF16),
                vmem((32, 512), BF16),
                vmem((384, WB), BF16),
                vmem((34 * 64, WB), BF16),
                vmem((34 * 64, WB), BF16),
                vmem((34 * 64, WB), BF16),
                vmem((HB * 64, WB), F32),
                vmem((4, 64, 128), F32),
                vmem((4, HB, WB), F32),
                vmem((HB, WB), F32),
                vmem((HB * 64, WB), BF16),
                vmem((136, 128), F32),
                vmem((3, 64, WB), F32),
                vmem((64, WB), F32),
                pltpu.SemaphoreType.DMA((11,)),
                pltpu.SemaphoreType.DMA((8,)),
                pltpu.SemaphoreType.DMA((8,)),
                pltpu.SemaphoreType.DMA((16,)),
                pltpu.SemaphoreType.DMA((18,)),
            ],
            compiler_params=pltpu.CompilerParams(
                collective_id=0, has_side_effects=True, vmem_limit_bytes=50*1024*1024
            ),
        )(*args)

    return jax.shard_map(
        on_device,
        mesh=mesh,
        in_specs=(
            P(None, ("grp", "ty"), "tx"),
            P(),
            P(),
            P(),
            P(),
            P(),
            P(),
            P(),
            P(("grp", "ty"), "tx", None),
            P(("grp", "ty"), "tx", None),
            P(None, ("grp", "ty"), "tx", None),
        ),
        out_specs=P(None, ("grp", "ty"), "tx"),
        check_vma=False,
    )
```

```python
import functools

import jax
import jax.numpy as jnp
from jax import lax
from jax.experimental import pallas as pl
from jax.experimental.pallas import tpu as pltpu
from jax.sharding import PartitionSpec as P

F32 = jnp.float32
BF16 = jnp.bfloat16
MESH = pl.DeviceIdType.MESH
NEAR = tuple((dr, dq) for dr in (-1, 0, 1) for dq in (-1, 0, 1) if (dr, dq) != (0, 0))
WIDE = tuple((dr, dq) for dr in (-2, -1, 0, 1, 2) for dq in (-1, 0, 1))
HB = 32
WB = 256
WE = 384
OWN = 9


def dot(a, b):
    return lax.dot_general(a, b, (((1,), (0,)), ((), ())), preferred_element_type=F32)


def dot_t(a, b):
    return lax.dot_general(a, b, (((1,), (1,)), ((), ())), preferred_element_type=F32)


def split2(x):
    high = x.astype(BF16)
    return high, (x - high.astype(F32)).astype(BF16)


def split3(x):
    high = x.astype(BF16)
    rest = x - high.astype(F32)
    middle = rest.astype(BF16)
    return high, middle, (rest - middle.astype(F32)).astype(BF16)


def kernel(
    n_rows,
    n_cols,
    n_ty,
    noisy_h, w_in_h, kf_h, wd_h, kc_h, wu_h, kl_h, wo_h, cell_h, count_h, obs_h,
    out_h,
    noisy_v, w_in_v, kf_v, wd_v, kc_v, wu_v, kl_v, wo_v, cell_v, count_v, obs_v,
    row_send, col_send, row_recv, col_recv, pool_send, pool_recv,
    ext, taps, taps_h, taps_l, a1, a2, enter_w, leave_w, wo8, expand, fine, fine_l, fine_r, acc, edge_ref,
    station_a, station_b, added, coarse, s_ref, raised_ref,
    in_sem, near_send, near_recv, wide_send, wide_recv,
):
    row = lax.axis_index("grp") * n_ty + lax.axis_index("ty")
    col = lax.axis_index("tx")

    row_of = {dr: (lax.div(row + dr, n_ty), lax.rem(row + dr, n_ty)) for dr in range(-2, 3)}

    def device(dr, dq):
        return row_of[dr] + (col + dq,)

    def row_ok(dr):
        return jnp.logical_and(row + dr >= 0, row + dr < n_rows)

    def col_ok(dq):
        return jnp.logical_and(col + dq >= 0, col + dq < n_cols)

    pairs = (
        (noisy_h, noisy_v), (w_in_h, w_in_v), (kf_h, kf_v), (kl_h, kl_v), (wo_h, wo_v), (cell_h, cell_v),
        (count_h, count_v), (obs_h, obs_v), (wd_h, wd_v), (wu_h, wu_v), (kc_h, kc_v),
    )
    loads = [pltpu.make_async_copy(src, dst, in_sem.at[k]) for k, (src, dst) in enumerate(pairs)]
    loads[0].start()

    def there(dr, dq):
        if dq == 0:
            return row_ok(dr)
        return col_ok(dq) if dr == 0 else jnp.logical_and(row_ok(dr), col_ok(dq))

    barrier = pltpu.get_barrier_semaphore()
    for dr, dq in WIDE:
        if (dr, dq) != (0, 0):

            @pl.when(there(dr, dq))
            def _(dr=dr, dq=dq):
                pl.semaphore_signal(barrier, inc=1, device_id=device(dr, dq), device_id_type=MESH)


    for load in loads[1:]:
        load.start()

    loads[0].wait()
    for v in range(4):
        row_send[0, 2 * v : 2 * v + 2, :] = noisy_v[v, 0:2, :]
        row_send[1, 2 * v : 2 * v + 2, :] = noisy_v[v, HB - 2 : HB, :]
    first = jnp.concatenate([noisy_v[v, :, 0:128] for v in range(4)], axis=0)
    last = jnp.concatenate([noisy_v[v, :, 128:256] for v in range(4)], axis=0)
    col_send[0] = first.T[0:8, :]
    col_send[1] = last.T[120:128, :]

    above_count = jnp.minimum(row, 2)
    below_count = jnp.minimum(n_rows - 1 - row, 2)
    sides = jnp.minimum(col, 1) + jnp.minimum(n_cols - 1 - col, 1)
    pl.semaphore_wait(barrier, (above_count + below_count + 1) * (sides + 1) - 1)
    near = []
    for k, (dr, dq) in enumerate(NEAR):
        if dq == 0:
            src = row_send.at[0 if dr < 0 else 1]
            dst = row_recv.at[1 if dr < 0 else 0]
        else:
            src = col_send.at[0 if dq < 0 else 1]
            dst = col_recv.at[1 if dq < 0 else 0, 1 - dr]
        back = NEAR.index((-dr, -dq))
        near.append(
            pltpu.make_async_remote_copy(
                src_ref=src, dst_ref=dst, send_sem=near_send.at[k], recv_sem=near_recv.at[back],
                device_id=device(dr, dq), device_id_type=MESH,
            )
        )
    for copy, (dr, dq) in zip(near, NEAR):
        pl.when(there(dr, dq))(copy.start)

    for load in loads[1:]:
        load.wait()
    w_tiled = dot_hi(w_in_v[...].T)
    lane = lax.broadcasted_iota(jnp.int32, (64, 128), 1)
    zero64 = jnp.zeros((64, 64), BF16)
    kf9 = jnp.concatenate([kf_v[p, q] for p in range(3) for q in range(3)], axis=1)
    for r in range(4):
        placed = []
        for p in range(3):
            for q in range(3):
                at = 12 * (r + p) + 4 * q
                placed.append(jnp.where(jnp.logical_and(lane >= at, lane < at + 4), w_tiled, 0.0))
        placed = jnp.concatenate(placed, axis=0)
        high, middle, low = split3(placed)
        conv = 0.5 * (dot(kf9, high) + dot(kf9, middle) + dot(kf9, low))
        at = 12 * (r + 1) + 4
        lift = jnp.where(jnp.logical_and(lane >= at, lane < at + 4), w_tiled, 0.0)
        high, low = split2(jnp.concatenate([conv, lift], axis=0))
        a1[r, :, 0:80] = high[:, 0:80]
        a1[r, :, 80:160] = high[:, 0:80]
        a1[r, :, 160:240] = low[:, 0:80]
    half = [[(kl_v[p, q].astype(F32) * 0.5).astype(BF16) for q in range(3)] for p in range(3)]
    for q in range(3):
        upper = jnp.concatenate([half[0][q], half[1][q], half[2][q], zero64], axis=1)
        lower = jnp.concatenate([zero64, half[0][q], half[1][q], half[2][q]], axis=1)
        a2[q] = jnp.concatenate([upper, lower], axis=0)
    stack = jnp.concatenate([half[p][q] for p in range(3) for q in range(3)], axis=0)
    leave_w[0:576] = dot(stack, wu_v[...]).astype(BF16)
    leave_w[576:640] = wu_v[...]
    down = jnp.concatenate([wd_v[...], jnp.zeros((64, 256), BF16)], axis=0)
    for p in range(3):
        for q in range(3):
            at = 128 * (3 * p + q)
            enter_w[at : at + 128] = dot_t(down, kc_v[p, q]).astype(BF16)
    pick = (lax.broadcasted_iota(jnp.int32, (32, 4), 0) // 8 == lax.broadcasted_iota(jnp.int32, (32, 4), 1))
    spread = dot(pick.astype(BF16), wo_v[...])
    spread = jnp.concatenate([spread] * 8, axis=1)
    same = lax.broadcasted_iota(jnp.int32, (32, 512), 0) % 8 == lax.broadcasted_iota(jnp.int32, (32, 512), 1) // 64
    wo8[...] = jnp.where(same, spread, 0.0).astype(BF16)
    place = lax.broadcasted_iota(jnp.int32, (128, WB), 0)
    pixel = lax.broadcasted_iota(jnp.int32, (128, WB), 1)
    for q in range(3):
        want = 7 + (pixel + (32 + q - 1)) // 32
        found = jnp.logical_and(place < 72, place % 24 == want)
        expand[128 * q : 128 * q + 128] = found.astype(F32).astype(BF16)

    cell = cell_v[0]
    count = count_v[0].astype(F32)
    at_row = (lax.broadcasted_iota(jnp.int32, (HB, 128), 0) == cell // WB).astype(F32)
    at_col = (lax.broadcasted_iota(jnp.int32, (WB, 128), 0) == cell % WB).astype(F32).astype(BF16)
    reports = [at_row * (count * obs_v[v, 0]) for v in range(4)] + [at_row * count]
    parts = split3(jnp.concatenate(reports, axis=0))
    sums = dot_t(parts[0], at_col) + dot_t(parts[1], at_col) + dot_t(parts[2], at_col)
    for v in range(4):
        station_a[v] = 0.5 * noisy_v[v] + 0.25 * sums[HB * v : HB * (v + 1)]
    station_b[...] = 0.5 - 0.25 * sums[HB * 4 :]

    ext[...] = jnp.zeros_like(ext)
    for v in range(4):
        ext[v, OWN : OWN + HB, 0:WB] = noisy_v[v]

    def make_taps(start, size):
        rows = slice(12 * start, 12 * (start + size))
        for v in range(4):
            left, right = ext[v, start : start + size, 0:128], ext[v, start : start + size, 128:256]
            spot = lax.broadcasted_iota(jnp.int32, left.shape, 1)
            up = [pltpu.roll(x, 1, 1) for x in (left, right)]
            down = [pltpu.roll(x, 127, 1) for x in (left, right)]
            shifted = (
                (jnp.where(spot < 1, 0.0, up[0]), left, jnp.where(spot < 127, down[0], down[1])),
                (jnp.where(spot < 1, up[0], up[1]), right, jnp.where(spot < 127, down[1], 0.0)),
            )
            for t in range(2):
                for q in range(3):
                    taps[t, pl.ds(12 * start + 4 * q + v, size, stride=12), :] = shifted[t][q]
        for t in range(2):
            high, low = split2(taps[t, rows])
            taps_h[rows, 128 * t : 128 * t + 128] = high
            taps_l[rows, 128 * t : 128 * t + 128] = low

    def make_side_taps(start, size):
        for v in range(4):
            rows = slice(start, start + size)
            spot = lax.broadcasted_iota(jnp.int32, (size, 128), 1)
            near_columns = jnp.where(
                spot < 4, pltpu.roll(ext[v, rows, 0:128], 2, 1), pltpu.roll(ext[v, rows, 128:256], 6, 1)
            )
            inside = jnp.logical_and(spot >= 2, spot < 6)
            here = jnp.where(inside, near_columns, ext[v, rows, WB:WE])
            for q, value in enumerate((pltpu.roll(here, 1, 1), here, pltpu.roll(here, 127, 1))):
                taps[2, pl.ds(12 * start + 4 * q + v, size, stride=12), :] = value

    def side_columns(k):
        right = jnp.where(jnp.logical_and(row_ok(k - 1), col_ok(1)), col_recv[1, k], 0.0)
        left = jnp.where(jnp.logical_and(row_ok(k - 1), col_ok(-1)), col_recv[0, k], 0.0)
        place = lax.broadcasted_iota(jnp.int32, (8, 128), 0)
        both = jnp.where(place < 2, pltpu.roll(left, 2, 0), jnp.where(place >= 6, pltpu.roll(right, 6, 0), 0.0))
        return jnp.concatenate([both, jnp.zeros((120, 128), F32)], axis=0).T

    def window(at):
        high = taps_h[pl.ds(at, 80), :]
        return jnp.concatenate([high, taps_l[pl.ds(at, 80), :], high], axis=0)

    def gated(both):
        h = both[0:64]
        return both[64:128] + (h + h * jnp.tanh(h))

    def fine_row(i, rhs, gate=None):
        value = gated(dot(a1[i % 4], rhs))
        if gate is not None:
            value = value * jnp.where(gate, 1.0, 0.0)
        fine[64 * (i + 1) : 64 * (i + 2), 0:WB] = value.astype(BF16)
        return value

    make_taps(0, 48)
    middle = jnp.zeros((64, WB), F32)
    for g in range(8):
        rhs = window(96 + 48 * g)
        for r in range(4):
            if 0 < 4 * g + r < HB - 1:
                middle = middle + fine_row(4 * g + r, rhs)

    lane = lax.broadcasted_iota(jnp.int32, (64, 128), 1)
    group, spot = lane // 8, lane % 8
    gate = jnp.where(spot == 1, jnp.where(col_ok(-1), 1.0, 0.0), jnp.where(spot == 6, jnp.where(col_ok(1), 1.0, 0.0), 1.0))
    gate = gate * jnp.where(group == 8, jnp.where(row_ok(-1), 1.0, 0.0), jnp.where(group == 9, jnp.where(row_ok(1), 1.0, 0.0), 1.0))
    starts = [96 + 48 * g for g in range(8)] + [48, 480]
    tap_lane = lax.broadcasted_iota(jnp.int32, (80, 128), 1) // 8

    def side_inputs(groups, packed):
        for g in groups:
            value = taps[2, pl.ds(starts[g], 80), :]
            packed = jnp.where(tap_lane == g, value if g == 0 else pltpu.roll(value, 8 * g, 1), packed)
        high, low = split2(packed)
        return packed, jnp.concatenate([high, low, high], axis=0)

    def side_rows(r, rhs):
        value = gated(dot(a1[r], rhs)) * gate
        edge_ref[r] = value
        return value

    pixel = lax.broadcasted_iota(jnp.int32, (8, WE), 1)
    cell_of = jnp.where(pixel < WB, pixel // 32, jnp.where(pixel % 8 == 2, 0, jnp.where(pixel % 8 == 5, 7, 8)))
    cell_of = jnp.where(jnp.logical_or(pixel == 0, pixel == WB - 1), 8, cell_of)
    into = (cell_of == lax.broadcasted_iota(jnp.int32, (8, WE), 0)).astype(F32).astype(BF16)

    def sums_of(upper, upper_side, lower, lower_side):
        stack = jnp.concatenate(
            [jnp.concatenate([upper, upper_side], axis=1), jnp.concatenate([lower, lower_side], axis=1)], axis=0
        )
        high, low = split2(stack)
        return (dot_t(into, high) + dot_t(into, low)) * (1.0 / 1024.0)

    for k, (dr, dq) in enumerate(NEAR):
        if dr >= 0:
            pl.when(there(-dr, -dq))(near[k].wait_recv)
    above, beside = side_columns(0), side_columns(1)
    for v in range(4):
        ext[v, OWN - 2 : OWN, 0:WB] = jnp.where(row_ok(-1), row_recv[0, 2 * v : 2 * v + 2, :], 0.0)
        ext[v, OWN - 2 : OWN, WB:WE] = above[HB * v + HB - 2 : HB * v + HB]
        ext[v, OWN : OWN + HB, WB:WE] = beside[HB * v : HB * (v + 1)]
    make_taps(0, 16)
    make_side_taps(0, 48)
    first_row = fine_row(0, window(96))
    outer_row = fine_row(-1, window(48), row_ok(-1))
    packed, rhs = side_inputs(range(10), jnp.zeros((80, 128), F32))
    side = [side_rows(r, rhs) for r in range(4)]
    inner_side = jnp.where(lane < 64, side[1] + side[2], 0.0)
    side_sum = inner_side + jnp.where(lane < 64, side[0], 0.0) + jnp.where(lane < 56, side[3], 0.0)
    outer_side = jnp.where(group == 8, side[3], 0.0)
    tile = sums_of(middle + first_row, side_sum, outer_row, outer_side)
    pool_send[0] = tile
    wide, wide_at = [], []

    def send(which, dr, dq, slot):
        wide.append(
            pltpu.make_async_remote_copy(
                src_ref=pool_send.at[which], dst_ref=pool_recv.at[slot], send_sem=wide_send.at[len(wide)],
                recv_sem=wide_recv.at[slot], device_id=device(dr, dq), device_id_type=MESH,
            )
        )
        pl.when(there(dr, dq))(wide[-1].start)
        wide_at.append((dr, dq))

    for dr in (1, 2):
        for dq in (-1, 0, 1):
            send(0, dr, dq, WIDE.index((-dr, -dq)))
    for dq in (-1, 1):
        send(0, 0, dq, WIDE.index((0, -dq)))
    pool_recv[WIDE.index((0, 0))] = tile

    for k, (dr, dq) in enumerate(NEAR):
        if dr < 0:
            pl.when(there(-dr, -dq))(near[k].wait_recv)
    below = side_columns(2)
    for v in range(4):
        ext[v, OWN + HB : OWN + HB + 2, 0:WB] = jnp.where(row_ok(1), row_recv[1, 2 * v : 2 * v + 2, :], 0.0)
        ext[v, OWN + HB : OWN + HB + 2, WB:WE] = below[HB * v : HB * v + 2]
    make_taps(40, 8)
    make_side_taps(40, 8)
    last_row = fine_row(HB - 1, window(432))
    outer_row = fine_row(HB, window(480), row_ok(1))
    packed, rhs = side_inputs((7, 9), packed)
    low_side, top_side = side_rows(3, rhs), side_rows(0, rhs)
    outer_side = jnp.where(group == 9, top_side, 0.0)
    inner_side = inner_side + jnp.where(lane < 64, low_side, 0.0)
    all_side = inner_side + jnp.where(lane < 64, top_side, 0.0)
    low_sum = inner_side + jnp.where(jnp.logical_and(lane >= 8, lane < 64), top_side, 0.0)
    pool_send[1] = sums_of(middle + last_row, low_sum, outer_row, outer_side)
    tile = sums_of(middle + first_row + last_row, all_side, outer_row, outer_side)
    pool_send[2] = tile
    for dr in (-1, -2):
        for dq in (-1, 0, 1):
            send(1, dr, dq, WIDE.index((-dr, -dq)))
    for dq in (-1, 1):
        send(2, 0, dq, 16 - dq)
    pool_recv[16] = tile

    for e in range(HB + 2):
        g = 8 if e == 0 else 9 if e == HB + 1 else (e - 1) // 4
        edge = edge_ref[(e - 1) % 4]
        rows = slice(64 * e, 64 * e + 64)
        left, right = fine[rows, 0:128].astype(F32), fine[rows, 128:256].astype(F32)
        up = [pltpu.roll(x, 1, 1) for x in (left, right)]
        down = [pltpu.roll(x, 127, 1) for x in (left, right)]
        turned = [pltpu.roll(edge, (at - 8 * g) % 128, 1) for at in (-1, -2, 122, 121)]
        fine_l[rows, 0:128] = jnp.where(lane < 2, turned[0], up[0]).astype(BF16)
        fine_l[rows, 128:256] = jnp.where(lane < 1, up[0], up[1]).astype(BF16)
        fine_r[rows, 0:128] = jnp.where(lane < 127, down[0], down[1]).astype(BF16)
        fine_r[rows, 128:256] = jnp.where(lane < 126, down[1], turned[3]).astype(BF16)
        fine[rows, 0:128] = jnp.where(lane < 1, turned[1], left).astype(BF16)
        fine[rows, 128:256] = jnp.where(lane < 127, right, turned[2]).astype(BF16)

    def last_rows(k, carry):
        at = pl.multiple_of(k * 128, 128)
        total = dot(a2[0], fine_l[pl.ds(at, 256), :])
        total += dot(a2[1], fine[pl.ds(at, 256), 0:WB])
        total += dot(a2[2], fine_r[pl.ds(at, 256), :])
        acc[pl.ds(at, 128), :] = total
        return carry

    lax.fori_loop(0, 16, last_rows, 0, unroll=True)
    for g in range(4):
        part = dot(wo8[...], fine[512 * g + 64 : 512 * g + 576, :])
        for v in range(4):
            rows = slice(8 * g, 8 * g + 8)
            station_a[v, rows, :] += station_b[rows, :] * part[8 * v : 8 * v + 8]

    for copy, (dr, dq) in zip(wide, wide_at):
        pl.when(there(-dr, -dq))(copy.wait_recv)
    cells = []
    for dr, dq in WIDE:
        if dr == 0:
            cell = pool_recv[16 + dq]
        else:
            step = 1 if dr > 0 else -1
            if dr == 1:
                other = pool_recv[16 + dq]
            else:
                other = pool_recv[WIDE.index((dr - step, dq))]
            cell = pool_recv[WIDE.index((dr, dq))] + pltpu.roll(other, 64, 1)
        cells.append(jnp.where(jnp.logical_and(row_ok(dr), col_ok(dq)), cell, 0.0))
    cells = jnp.concatenate(cells, axis=0)
    coarse[0:8] = jnp.zeros((8, 128), F32)
    coarse[128:136] = jnp.zeros((8, 128), F32)
    coarse[8:128] = cells
    around = jnp.concatenate(
        [coarse[8 + 24 * p + q - 1 : 80 + 24 * p + q - 1].astype(BF16) for p in range(3) for q in range(3)], axis=1
    )
    h = 0.5 * dot(around, enter_w[...])
    leaving = dot(cells[24:96, 0:64].astype(BF16), wd_v[...]) + (h + h * jnp.tanh(h))
    blocks = []
    for k, (dr, dq) in enumerate(WIDE[3:12]):
        block = leaving[8 * k : 8 * k + 8]
        blocks.append(jnp.where(jnp.logical_and(row_ok(dr), col_ok(dq)), block, 0.0))
    leaving = jnp.concatenate(blocks + [jnp.zeros((56, 256), F32)], axis=0).astype(BF16)
    parts = dot_t(leave_w[...], leaving)
    cell_lane = lax.broadcasted_iota(jnp.int32, (64, 128), 1)
    inside = jnp.logical_and(cell_lane >= 24, cell_lane < 48)
    mixed = []
    raised = jnp.where(inside, parts[576:640], 0.0)
    none = jnp.zeros((64, 128), F32)
    raised_low = raised - raised.astype(BF16).astype(F32)
    for q in range(3):
        one, two, three = (parts[64 * (3 * p + q) : 64 * (3 * p + q) + 64] for p in range(3))
        mixed.append(
            jnp.concatenate(
                [
                    jnp.where(cell_lane < 24, one, jnp.where(inside, two + three, 0.0)),
                    jnp.where(inside, one + two + three, 0.0),
                    jnp.where(inside, one + two, jnp.where(cell_lane >= 48, three, 0.0)),
                    raised if q == 1 else none,
                    raised_low if q == 1 else none,
                ],
                axis=0,
            ).astype(BF16)
        )
    spread = dot(jnp.concatenate(mixed, axis=1), expand[...])
    for edge in range(3):
        s_ref[edge] = spread[64 * edge : 64 * edge + 64]
    raised_ref[...] = spread[192:256] + spread[256:320]

    def finish(i, edge):
        at = i * 64 if isinstance(i, int) else pl.multiple_of(i * 64, 64)
        h = acc[pl.ds(at, 64), :] + s_ref[edge]
        value = raised_ref[...] + (h + h * jnp.tanh(h))
        added[pl.ds(at, 64), :] = value.astype(BF16)

    def finish_middle(i, carry):
        finish(i, 1)
        return carry

    finish(0, 0)
    finish(HB - 1, 2)
    lax.fori_loop(1, HB - 1, finish_middle, 0, unroll=True)
    for g in range(4):
        denoised = dot(wo8[...], added[512 * g : 512 * g + 512, :])
        for v in range(4):
            rows = slice(8 * g, 8 * g + 8)
            out_h[v, rows, :] = station_a[v, rows, :] + station_b[rows, :] * denoised[8 * v : 8 * v + 8]
    for copy, (dr, dq) in zip(wide + near, wide_at + list(NEAR)):
        pl.when(there(dr, dq))(copy.wait_send)


def dot_hi(w_in):
    place = lax.broadcasted_iota(jnp.int32, (4, 128), 1) % 4 == lax.broadcasted_iota(jnp.int32, (4, 128), 0)
    place = place.astype(F32).astype(BF16)
    high, middle, low = split3(w_in)
    return (dot(high, place) + dot(middle, place)) + dot(low, place)


def solution(mesh):
    n_ty = mesh.shape["ty"]
    n_rows = mesh.shape["grp"] * n_ty
    n_cols = mesh.shape["tx"]

    def on_device(noisy, w_in, kf, wd, kc, wu, kl, wo, cell, count, obs):
        w_in, wd = w_in.T, wd.T
        obs = obs.reshape(4, 1, 128)
        cell = cell.reshape(1, 1, 128)
        count = count.reshape(1, 1, 128)
        args = (noisy, w_in, kf, wd, kc, wu, kl, wo, cell, count, obs)
        vmem = pltpu.VMEM
        args = tuple(pltpu.with_memory_space_constraint(x, pltpu.HBM) for x in args)
        return pl.pallas_call(
            functools.partial(kernel, n_rows, n_cols, n_ty),
            out_shape=jax.ShapeDtypeStruct(noisy.shape, noisy.dtype),
            in_specs=[pl.BlockSpec(memory_space=pltpu.HBM)] * 11,
            out_specs=pl.BlockSpec(memory_space=pltpu.VMEM),
            scratch_shapes=[vmem(x.shape, x.dtype) for x in args]
            + [
                vmem((2, 8, WB), F32),
                vmem((2, 8, 128), F32),
                vmem((2, 8, WB), F32),
                vmem((2, 3, 8, 128), F32),
                vmem((3, 8, 128), F32),
                vmem((18, 8, 128), F32),
                vmem((4, 48, WE), F32),
                vmem((3, 576, 128), F32),
                vmem((576, WB), BF16),
                vmem((576, WB), BF16),
                vmem((4, 128, 240), BF16),
                vmem((3, 128, 256), BF16),
                vmem((1152, 256), BF16),
                vmem((640, 256), BF16),
                vmem((32, 512), BF16),
                vmem((384, WB), BF16),
                vmem((34 * 64, WB), BF16),
                vmem((34 * 64, WB), BF16),
                vmem((34 * 64, WB), BF16),
                vmem((HB * 64, WB), F32),
                vmem((4, 64, 128), F32),
                vmem((4, HB, WB), F32),
                vmem((HB, WB), F32),
                vmem((HB * 64, WB), BF16),
                vmem((136, 128), F32),
                vmem((3, 64, WB), F32),
                vmem((64, WB), F32),
                pltpu.SemaphoreType.DMA((11,)),
                pltpu.SemaphoreType.DMA((8,)),
                pltpu.SemaphoreType.DMA((8,)),
                pltpu.SemaphoreType.DMA((16,)),
                pltpu.SemaphoreType.DMA((18,)),
            ],
            compiler_params=pltpu.CompilerParams(
                collective_id=0, has_side_effects=True, vmem_limit_bytes=50*1024*1024
            ),
        )(*args)

    return jax.shard_map(
        on_device,
        mesh=mesh,
        in_specs=(
            P(None, ("grp", "ty"), "tx"),
            P(),
            P(),
            P(),
            P(),
            P(),
            P(),
            P(),
            P(("grp", "ty"), "tx", None),
            P(("grp", "ty"), "tx", None),
            P(None, ("grp", "ty"), "tx", None),
        ),
        out_specs=P(None, ("grp", "ty"), "tx"),
        check_vma=False,
    )
```
